8 devices in a mesh: dp: 1 (over z), ep: 8 (over y, x, core).
Axes of the slice: x: 2, y: 2, z: 1, core: 2. Of those that a mesh axis runs over, the one named last changes fastest.
Arguments:
- tokens: bfloat16 [2048, 2048], P(('dp', 'ep'))
- logits: float32 [2048, 256], P(('dp', 'ep'))
- w_in: bfloat16 [256, 2048, 512], P('ep')
- w_out: bfloat16 [256, 512, 2048], P('ep')
Outputs:
- output: bfloat16 [2048, 2048], P(('dp', 'ep'))
All inputs are finite; a program needn't handle non-finite values.
Results may differ from the reference program's by a relative error of at most 0.001.
Values are sent between devices in bfloat16 or wider.
A program may use at most 1 GiB of HBM per device.

```python
import jax
import jax.numpy as jnp
from jax import lax

TOKENS_DEV = 256
GROUP = 8
D_MODEL = 2048
FF = 512
EXPERTS = 256
CAP_FACTOR = 2

NUM_TOK = TOKENS_DEV * GROUP
CAPACITY = NUM_TOK * CAP_FACTOR // EXPERTS
HALF_CAP = CAPACITY // 2
QUARTER_CAP = CAPACITY // 4
OTHER_TOK = (GROUP - 2) * TOKENS_DEV
SPACING = max(1, 1024 // CAPACITY)


def row_perms(key, rows, width):
    base = jnp.broadcast_to(jnp.arange(width, dtype=jnp.int32), (rows, width))
    return jax.random.permutation(key, base, axis=1, independent=True)


def route_logits(key):
    keys = jax.random.split(key, 6)
    first_src = jax.random.randint(keys[0], (EXPERTS, 1), 0, GROUP)
    second_src = (first_src + jax.random.randint(keys[1], (EXPERTS, 1), 1, GROUP)) % GROUP
    local_perm = row_perms(keys[2], EXPERTS * GROUP, TOKENS_DEV).reshape(EXPERTS, NUM_TOK)
    other_perm = row_perms(keys[3], EXPERTS, OTHER_TOK)
    mix_perm = row_perms(keys[4], EXPERTS, CAPACITY)
    low_perm = row_perms(keys[5], EXPERTS, NUM_TOK)
    token_ids = jnp.arange(NUM_TOK, dtype=jnp.int32)[None, :]
    source = token_ids // TOKENS_DEV
    local = token_ids % TOKENS_DEV
    on_first = source == first_src
    on_second = source == second_src
    packed = source - (source > first_src).astype(jnp.int32) - (source > second_src).astype(jnp.int32)
    other_rank = jnp.take_along_axis(other_perm, jnp.clip(packed * TOKENS_DEV + local, 0, OTHER_TOK - 1), axis=1)
    level = jnp.where(on_first, local_perm, jnp.where(on_second, HALF_CAP + local_perm, HALF_CAP + QUARTER_CAP + other_rank))
    chosen = jnp.where(on_first, local_perm < HALF_CAP, jnp.where(on_second, local_perm < QUARTER_CAP, other_rank < QUARTER_CAP))
    mixed = jnp.take_along_axis(mix_perm, jnp.clip(level, 0, CAPACITY - 1), axis=1)
    int_logit = jnp.where(chosen, 2048 + SPACING * mixed, -1 - low_perm)
    return (int_logit.astype(jnp.float32) / 1024.0).T


def setup_inputs(seed: int = 0, part: int = 0) -> dict:
    key = jax.random.key(seed)
    key_tok = jax.random.fold_in(jax.random.fold_in(key, 1), part)
    key_route = jax.random.fold_in(jax.random.fold_in(key, 2), part)
    key_in, key_out = jax.random.split(jax.random.fold_in(key, 3))
    tokens = jax.random.normal(key_tok, (NUM_TOK, D_MODEL), jnp.float32).astype(jnp.bfloat16)
    logits = route_logits(key_route)
    w_in = (jax.random.normal(key_in, (EXPERTS, D_MODEL, FF), jnp.float32) * D_MODEL ** -0.5).astype(jnp.bfloat16)
    w_out = (jax.random.normal(key_out, (EXPERTS, FF, D_MODEL), jnp.float32) * (1.5 * FF ** -0.5)).astype(jnp.bfloat16)
    return {"tokens": tokens, "logits": logits, "w_in": w_in, "w_out": w_out}


def expert_ffn(operands):
    rows, w_in_e, w_out_e = operands
    hidden = jax.nn.gelu(jnp.dot(rows, w_in_e, preferred_element_type=jnp.float32), approximate=False).astype(jnp.bfloat16)
    return jnp.dot(hidden, w_out_e, preferred_element_type=jnp.float32).astype(jnp.bfloat16)


def reference(tokens, logits, w_in, w_out):
    gates = jax.nn.softmax(logits, axis=-1)
    top_idx = lax.top_k(logits.T, CAPACITY)[1]
    picked = tokens[top_idx]
    expert_out = lax.map(expert_ffn, (picked, w_in, w_out))
    sel_gate = jnp.take_along_axis(gates.T, top_idx, axis=1)
    weighted = sel_gate[:, :, None] * expert_out.astype(jnp.float32)
    combined = jax.ops.segment_sum(weighted.reshape(-1, D_MODEL), top_idx.reshape(-1), num_segments=NUM_TOK)
    return (tokens.astype(jnp.float32) + combined).astype(jnp.bfloat16)
```

```python
import functools

import jax
import jax.numpy as jnp
from jax import lax
from jax.experimental import pallas as pl
from jax.experimental.pallas import tpu as pltpu
from jax.sharding import PartitionSpec as P

MESH = pl.DeviceIdType.MESH
F32, BF16 = jnp.float32, jnp.bfloat16
DEV = 8
TOK = 256
D = 2048
FF = 512
EXP = 32
ALL_EXP = EXP * DEV
CAP = 16
SLOTS = EXP * CAP
NC = 8
CW = D // NC
GE = 8
NG = EXP // GE
ITEMS = NC * NG


def dot(a, b):
    return jnp.dot(a, b, preferred_element_type=F32)


def iota(shape, dim):
    return lax.broadcasted_iota(jnp.int32, shape, dim)


def gelu(v):
    return 0.5 * v * (1.0 + lax.erf(v * 0.7071067811865476))


def moe_kernel(bound, ns1, ns2, tok, logit, w1, w2, out, flag_out,
               xall, w1buf, w2buf, lt, ltr, thr_own, thr, n_own, n_par, flag_own, flags,
               slot_s, rank_s, p_s, v_s, vt_s, q_s, pick_s, hacc, h_s, zc_s, zs, recv,
               r2_s, gt_s, at_s, a_s, out_s,
               w1sem, w2sem, xsem, osem, lsend, lrecv, tsend, trecv, fsend, frecv, nsem,
               dsend, drecv, rsend, rrecv):
    me = lax.axis_index("ep")
    k = me % 2
    chip = me // 2
    cx = chip % 2
    cy = chip // 2
    dx = 2 - 4 * cx
    dy = 4 - 8 * cy
    other = 1 - 2 * k
    partner = me + other
    xn, yn, dg = me + dx, me + dy, me + dx + dy
    first = me + (1 - k) * dx + k * dy
    second = me + k * dx + (1 - k) * dy

    def rcopy(src, dst, ss, rs, dev):
        return pltpu.make_async_remote_copy(src_ref=src, dst_ref=dst, send_sem=ss, recv_sem=rs,
                                            device_id={"ep": dev}, device_id_type=MESH)

    def w1_copy(i):
        s = i % ns1
        return pltpu.make_async_copy(
            w1.at[pl.ds((i % NG) * GE, GE), pl.ds((i // NG) * CW, CW), :], w1buf.at[s], w1sem.at[s])

    def w2_copy(i):
        s = i % ns2
        return pltpu.make_async_copy(
            w2.at[pl.ds((i % NG) * GE, GE), :, pl.ds((i // NG) * CW, CW)], w2buf.at[s], w2sem.at[s])

    def x_copy(c):
        return pltpu.make_async_copy(tok.at[:, pl.ds(c * CW, CW)], xall.at[c, pl.ds(me * TOK, TOK), :], xsem.at[c])

    for c in range(NC):
        x_copy(c).start()
    for i in range(ns1):
        w1_copy(i).start()
    for i in range(ns2):
        w2_copy(i).start()

    barrier = pltpu.get_barrier_semaphore()
    for j in range(1, DEV):
        pl.semaphore_signal(barrier, inc=1, device_id={"ep": (me + j) % DEV}, device_id_type=MESH)
    lt[...] = logit[...].T
    ltr[pl.ds(me * EXP, EXP), :] = lt[pl.ds(me * EXP, EXP), :]
    pl.semaphore_wait(barrier, DEV - 1)

    def l_copy(j):
        d = (me + j) % DEV
        return rcopy(lt.at[pl.ds(d * EXP, EXP), :], ltr.at[pl.ds(me * EXP, EXP), :], lsend.at[j], lrecv.at[me], d)

    for j in range(1, DEV):
        l_copy(j).start()

    def xblk(c, d):
        return xall.at[c, pl.ds(d * TOK, TOK), :]

    def d_copy(c, block, dev, n):
        return rcopy(xblk(c, block), xblk(c, block), dsend.at[c * 7 + n], drecv.at[c * DEV + block], dev)

    def own(c):
        x_copy(c).wait()
        d_copy(c, me, first, 0).start()
        d_copy(c, me, second, 1).start()
        d_copy(c, me, partner, 2).start()

    def pump(c):
        d_copy(c, first, partner, 4).wait_recv()
        d_copy(c, first, second, 3).start()
        d_copy(c, first, partner, 4).start()

        @pl.when(c + 2 < NC)
        def _():
            own(c + 2)

        d_copy(c, second, partner, 5).wait_recv()
        d_copy(c, second, partner, 5).start()
        d_copy(c, dg, partner, 6).wait_recv()
        d_copy(c, dg, partner, 6).start()

    def partner_blocks(c):
        for d in (partner, first + other, second + other, dg + other):
            d_copy(c, d, partner, 0).wait_recv()

    own(0)
    own(1)

    for j in range(1, DEV):
        s = (me + j) % DEV
        rcopy(lt.at[pl.ds(0, EXP), :], ltr.at[pl.ds(s * EXP, EXP), :], lsend.at[j], lrecv.at[s], s).wait_recv()
    neg = jnp.float32(-jnp.inf)

    def next_max(_, m):
        acc = jnp.full((EXP, TOK), neg, F32)
        for s in range(DEV):
            v = ltr[s * EXP:(s + 1) * EXP, :]
            acc = jnp.maximum(acc, jnp.where(v < m, v, neg))
        return jnp.max(acc, axis=1, keepdims=True)

    t = lax.fori_loop(0, CAP, next_max, jnp.full((EXP, 1), jnp.inf, F32))
    thr_own[...] = jnp.broadcast_to(t, (EXP, 128))
    thr[pl.ds(me * EXP, EXP), :] = jnp.broadcast_to(t, (EXP, 128))

    def t_copy(j, src_dev):
        return rcopy(thr_own, thr.at[pl.ds(src_dev * EXP, EXP), :], tsend.at[j], trecv.at[src_dev], (me + j) % DEV)

    for j in range(1, DEV):
        t_copy(j, me).start()

    pump(0)

    tri = jnp.where(iota((TOK, TOK), 0) < iota((TOK, TOK), 1), 1.0, 0.0).astype(BF16)
    ones = jnp.ones((TOK, TOK), BF16)
    i0, i1 = iota((ALL_EXP, ALL_EXP), 0), iota((ALL_EXP, ALL_EXP), 1)
    s0, e0, s1, e1 = i0 >> 5, i0 & 31, i1 >> 5, i1 & 31
    t8 = jnp.concatenate([t] * DEV, axis=0)
    sel = ltr[...] >= t8
    mo = jnp.where(sel, 1.0, 0.0).astype(BF16)
    cnt = dot(mo, tri)
    num = dot(mo, ones).astype(BF16)
    m_slot = jnp.where((e0 == e1) & (s1 < s0), 1.0, 0.0).astype(BF16)
    m_rank = jnp.where(((s0 >> 1) == (s1 >> 1)) & ((e1 < e0) | ((e1 == e0) & (s1 < s0))), 1.0, 0.0).astype(BF16)
    slot_s[...] = jnp.where(sel, dot(m_slot, num) + cnt, -1.0)
    rank_s[...] = jnp.where(sel, dot(m_rank, num) + cnt, -1.0)

    kio = iota((CAP, TOK), 0).astype(F32)
    lio = iota((CAP, 128), 1)

    def build_p(e, _):
        acc = jnp.zeros((CAP, 128), F32)
        for ch in range(DEV // 2):
            v = jnp.zeros((CAP, TOK), F32)
            for s in (2 * ch, 2 * ch + 1):
                hit = slot_s[pl.ds(s * EXP + e, 1), :] == kio
                p_s[pl.ds(e * CAP, CAP), s * TOK:(s + 1) * TOK] = jnp.where(hit, 1.0, 0.0).astype(BF16)
                v = v + jnp.where(hit, rank_s[pl.ds(s * EXP + e, 1), :] + 1.0, 0.0)
            acc = jnp.where(lio == ch, jnp.sum(v, axis=1, keepdims=True), acc)
        v_s[pl.ds(e * CAP, CAP), :] = acc
        return 0

    lax.fori_loop(0, EXP, build_p, 0, unroll=2)
    pump(1)

    for j in range(1, DEV):
        t_copy(j, (me + j) % DEV).wait_recv()
    la = lt[...]
    sel2 = la >= jnp.concatenate([thr[...], thr[...]], axis=1)
    mt = jnp.where(sel2, 1.0, 0.0).astype(BF16)
    num2 = dot(mt, ones)
    n_own[...] = num2[:, :128]
    n_copy = rcopy(n_own, n_par, nsem.at[0], nsem.at[1], partner)
    n_copy.start()
    ex = jnp.exp(la - jnp.max(la, axis=0, keepdims=True))
    gt_s[...] = ex / jnp.sum(ex, axis=0, keepdims=True)

    vt_s[...] = v_s[...].T
    rio = iota((bound, SLOTS), 0).astype(F32) + 1.0
    for n, d in enumerate((xn, yn, dg, me)):
        q_s[n * bound:(n + 1) * bound, :] = jnp.where(vt_s[pl.ds(d // 2, 1), :] == rio, 1.0, 0.0).astype(BF16)

    n_copy.wait_recv()
    npar = jnp.concatenate([n_par[...], n_par[...]], axis=1)
    both = num2 + npar
    m_base = jnp.where((s0 == s1) & (e1 < e0), 1.0, 0.0).astype(BF16)
    base = dot(m_base, both.astype(BF16))
    r2_s[...] = jnp.where(sel2, base + dot(mt, tri) + k.astype(F32) * npar, -1.0)
    over = jnp.max(jnp.max(base + both, axis=0, keepdims=True), axis=1, keepdims=True)
    flag_own[...] = jnp.broadcast_to(jnp.where(over > bound, 1.0, 0.0), (8, 128))

    def f_copy(j, src_dev):
        return rcopy(flag_own, flags.at[src_dev], fsend.at[j], frecv.at[src_dev], (me + j) % DEV)

    for j in range(1, DEV):
        f_copy(j, me).start()
    flags[me] = flag_own[...]
    pump(2)
    hacc[...] = jnp.zeros((SLOTS, FF), F32)

    def first_product(c, last):
        partner_blocks(c)
        pick_s[...] = dot(p_s[...], xall[c]).astype(BF16)

        def group(g, _):
            i = c * NG + g
            w1_copy(i).wait()
            s = i % ns1
            for j in range(GE):
                rows = pl.ds(g * (GE * CAP) + j * CAP, CAP)
                v = hacc[rows, :] + dot(pick_s[rows, :], w1buf[s, j])
                if last:
                    h_s[rows, :] = gelu(v).astype(BF16)
                else:
                    hacc[rows, :] = v

            @pl.when(i + ns1 < ITEMS)
            def _():
                w1_copy(i + ns1).start()

            return 0

        lax.fori_loop(0, NG, group, 0)

    def early(c, _):
        first_product(c, False)
        return 0

    def later(c, _):
        pump(c)
        first_product(c, False)
        return 0

    lax.fori_loop(0, 3, early, 0)
    lax.fori_loop(3, NC - 1, later, 0)
    pump(NC - 1)
    first_product(NC - 1, True)

    def rblk(c, d):
        return recv.at[c, pl.ds(d * bound, bound), :]

    def z_copy(c, n, dev):
        src = rblk(c, me) if n == 3 else zs.at[c, pl.ds(n * bound, bound), :]
        return rcopy(src, rblk(c, me), rsend.at[c * 7 + n], rrecv.at[c * DEV + me], dev)

    def fwd_copy(c, n, block):
        return rcopy(rblk(c, block), rblk(c, block), rsend.at[c * 7 + 4 + n], rrecv.at[c * DEV + block], partner)

    def second_product(c, _):
        def group(g, _):
            i = c * NG + g
            w2_copy(i).wait()
            s = i % ns2
            for j in range(GE):
                rows = pl.ds(g * (GE * CAP) + j * CAP, CAP)
                zc_s[rows, :] = dot(h_s[rows, :], w2buf[s, j]).astype(BF16)

            @pl.when(i + ns2 < ITEMS)
            def _():
                w2_copy(i + ns2).start()

            return 0

        lax.fori_loop(0, NG, group, 0)
        zc = zc_s[...]
        zs[c] = dot(q_s[:3 * bound, :], zc).astype(BF16)
        recv[c, pl.ds(me * bound, bound), :] = dot(q_s[3 * bound:, :], zc).astype(BF16)
        for n, dev in ((2, dg), (0, xn), (1, yn), (3, partner)):
            z_copy(c, n, dev).start()
        return 0

    lax.fori_loop(0, NC, second_product, 0)

    RB = 64

    def build_a(n, _):
        o = n // (bound // RB)
        r0 = (n % (bound // RB)) * RB
        rio2 = (iota((RB, TOK), 0) + r0).astype(F32)

        def one(e, acc):
            row = pl.ds(o * EXP + e, 1)
            return jnp.where(r2_s[row, :] == rio2, gt_s[row, :], acc)

        at_s[pl.ds(o * bound + r0, RB), :] = lax.fori_loop(0, EXP, one, jnp.zeros((RB, TOK), F32), unroll=8)
        return 0

    lax.fori_loop(0, DEV * (bound // RB), build_a, 0)

    def split_a(j, _):
        a = at_s[pl.ds(j * 128, 128), :].T
        for n in range(3):
            part = a.astype(BF16)
            a_s[n, :, pl.ds(j * 128, 128)] = part
            a = a - part.astype(F32)
        return 0

    lax.fori_loop(0, DEV * bound // 128, split_a, 0)

    def forward(c):
        for n, d in enumerate((xn, yn, dg)):
            fwd_copy(c, n, d).wait_recv()
            fwd_copy(c, n, d).start()

    def out_copy(c):
        return pltpu.make_async_copy(out_s.at[c], out.at[:, pl.ds(c * CW, CW)], osem.at[c])

    def combine(c):
        for d in (partner, xn + other, yn + other, dg + other):
            fwd_copy(c, 0, d).wait_recv()
        z = recv[c]
        y = dot(a_s[2], z) + dot(a_s[1], z) + dot(a_s[0], z)
        out_s[c] = (xall[c, pl.ds(me * TOK, TOK), :].astype(F32) + y).astype(BF16)
        out_copy(c).start()

    forward(0)

    def step(c, _):
        forward(c + 1)
        combine(c)
        return 0

    lax.fori_loop(0, NC - 1, step, 0)
    combine(NC - 1)

    acc = flag_own[...]
    for j in range(1, DEV):
        s = (me + j) % DEV
        f_copy(j, s).wait_recv()
        acc = jnp.maximum(acc, flags[s])
    flag_out[...] = acc

    for j in range(1, DEV):
        l_copy(j).wait_send()
        t_copy(j, me).wait_send()
        f_copy(j, me).wait_send()
    n_copy.wait_send()

    def drain(c, _):
        for n, (block, dev) in enumerate(((me, first), (me, second), (me, partner), (first, second),
                                          (first, partner), (second, partner), (dg, partner))):
            d_copy(c, block, dev, n).wait_send()
        for n, dev in enumerate((xn, yn, dg, partner)):
            z_copy(c, n, dev).wait_send()
        for n, d in enumerate((xn, yn, dg)):
            fwd_copy(c, n, d).wait_send()
        out_copy(c).wait()
        return 0

    lax.fori_loop(0, NC, drain, 0)


def moe_call(bound, ns1, ns2, cid, tok, logit, w1, w2):
    vm = pltpu.VMEM
    sem = pltpu.SemaphoreType.DMA
    return pl.pallas_call(
        functools.partial(moe_kernel, bound, ns1, ns2),
        out_shape=(jax.ShapeDtypeStruct((TOK, D), BF16), jax.ShapeDtypeStruct((8, 128), F32)),
        in_specs=[pl.BlockSpec(memory_space=pl.ANY), pl.BlockSpec(memory_space=pltpu.VMEM),
                  pl.BlockSpec(memory_space=pl.ANY), pl.BlockSpec(memory_space=pl.ANY)],
        out_specs=(pl.BlockSpec(memory_space=pl.ANY), pl.BlockSpec(memory_space=pltpu.VMEM)),
        scratch_shapes=[
            vm((NC, DEV * TOK, CW), BF16), vm((ns1, GE, CW, FF), BF16), vm((ns2, GE, FF, CW), BF16),
            vm((ALL_EXP, TOK), F32), vm((ALL_EXP, TOK), F32), vm((EXP, 128), F32), vm((ALL_EXP, 128), F32),
            vm((ALL_EXP, 128), F32), vm((ALL_EXP, 128), F32), vm((8, 128), F32), vm((DEV, 8, 128), F32),
            vm((ALL_EXP, TOK), F32), vm((ALL_EXP, TOK), F32), vm((SLOTS, DEV * TOK), BF16),
            vm((SLOTS, 128), F32), vm((128, SLOTS), F32), vm((4 * bound, SLOTS), BF16),
            vm((SLOTS, CW), BF16), vm((SLOTS, FF), F32), vm((SLOTS, FF), BF16), vm((SLOTS, CW), BF16),
            vm((NC, 3 * bound, CW), BF16), vm((NC, DEV * bound, CW), BF16),
            vm((ALL_EXP, TOK), F32), vm((ALL_EXP, TOK), F32), vm((DEV * bound, TOK), F32),
            vm((3, TOK, DEV * bound), BF16), vm((NC, TOK, CW), BF16),
            sem((ns1,)), sem((ns2,)), sem((NC,)), sem((NC,)), sem((DEV,)), sem((DEV,)), sem((DEV,)), sem((DEV,)),
            sem((DEV,)), sem((DEV,)), sem((2,)), sem((NC * 7,)), sem((NC * DEV,)), sem((NC * 7,)), sem((NC * DEV,)),
        ],
        compiler_params=pltpu.CompilerParams(collective_id=cid, has_side_effects=True, vmem_limit_bytes=67043328),
        name=f"moe_{bound}",
    )(tok, logit, w1, w2)


def solution(mesh):
    row_spec = P(("dp", "ep"), None)
    expert_spec = P("ep", None, None)

    def device_step(tok, logit, w1, w2):
        out, flag = moe_call(192, 5, 8, 0, tok, logit, w1, w2)
        return lax.cond(flag[0, 0] > 0, lambda: moe_call(512, 2, 2, 1, tok, logit, w1, w2)[0], lambda: out)

    return jax.shard_map(device_step, mesh=mesh, in_specs=(row_spec, row_spec, expert_spec, expert_spec),
                         out_specs=row_spec, check_vma=False)
```

```python
import functools

import jax
import jax.numpy as jnp
from jax import lax
from jax.experimental import pallas as pl
from jax.experimental.pallas import tpu as pltpu
from jax.sharding import PartitionSpec as P

MESH = pl.DeviceIdType.MESH
F32, BF16 = jnp.float32, jnp.bfloat16
DEV = 8
TOK = 256
D = 2048
FF = 512
EXP = 32
ALL_EXP = EXP * DEV
CAP = 16
SLOTS = EXP * CAP
NC = 8
CW = D // NC
GE = 8
NG = EXP // GE
ITEMS = NC * NG


def dot(a, b):
    return jnp.dot(a, b, preferred_element_type=F32)


def iota(shape, dim):
    return lax.broadcasted_iota(jnp.int32, shape, dim)


def gelu(v):
    return 0.5 * v * (1.0 + lax.erf(v * 0.7071067811865476))


def moe_kernel(bound, ns1, ns2, tok, logit, w1, w2, out, flag_out,
               xall, w1buf, w2buf, log_s, lt, ltr, thr_own, thr, n_own, n_par, flag_own, flags,
               slot_s, rank_s, p_s, v_s, vt_s, q_s, pick_s, hacc, h_s, zc_s, zs, recv,
               r2_s, gt_s, at_s, a_s, out_s,
               w1sem, w2sem, xsem, osem, lsend, lrecv, tsend, trecv, fsend, frecv, nsem,
               dsend, drecv, rsend, rrecv):
    me = lax.axis_index("ep")
    k = me % 2
    chip = me // 2
    cx = chip % 2
    cy = chip // 2
    dx = 2 - 4 * cx
    dy = 4 - 8 * cy
    other = 1 - 2 * k
    partner = me + other
    xn, yn, dg = me + dx, me + dy, me + dx + dy
    first = me + (1 - k) * dx + k * dy
    second = me + k * dx + (1 - k) * dy

    def rcopy(src, dst, ss, rs, dev):
        return pltpu.make_async_remote_copy(src_ref=src, dst_ref=dst, send_sem=ss, recv_sem=rs,
                                            device_id={"ep": dev}, device_id_type=MESH)

    def w1_copy(i):
        s = i % ns1
        return pltpu.make_async_copy(
            w1.at[pl.ds((i % NG) * GE, GE), pl.ds((i // NG) * CW, CW), :], w1buf.at[s], w1sem.at[s])

    def w2_copy(i):
        s = i % ns2
        return pltpu.make_async_copy(
            w2.at[pl.ds((i % NG) * GE, GE), :, pl.ds((i // NG) * CW, CW)], w2buf.at[s], w2sem.at[s])

    def x_copy(c):
        return pltpu.make_async_copy(tok.at[:, pl.ds(c * CW, CW)], xall.at[c, pl.ds(me * TOK, TOK), :], xsem.at[c])

    barrier = pltpu.get_barrier_semaphore()
    for j in range(1, DEV):
        pl.semaphore_signal(barrier, inc=1, device_id={"ep": (me + j) % DEV}, device_id_type=MESH)
    log_copy = pltpu.make_async_copy(logit, log_s, nsem.at[2])
    log_copy.start()
    for c in range(NC):
        x_copy(c).start()
    log_copy.wait()
    lt[...] = log_s[...].T
    ltr[pl.ds(me * EXP, EXP), :] = lt[pl.ds(me * EXP, EXP), :]
    pl.semaphore_wait(barrier, DEV - 1)

    def l_copy(j):
        d = (me + j) % DEV
        return rcopy(lt.at[pl.ds(d * EXP, EXP), :], ltr.at[pl.ds(me * EXP, EXP), :], lsend.at[j], lrecv.at[me], d)

    for j in range(1, DEV):
        l_copy(j).start()

    def xblk(c, d):
        return xall.at[c, pl.ds(d * TOK, TOK), :]

    def d_copy(c, block, dev, n):
        return rcopy(xblk(c, block), xblk(c, block), dsend.at[c * 7 + n], drecv.at[c * DEV + block], dev)

    def own(c):
        x_copy(c).wait()
        d_copy(c, me, first, 0).start()
        d_copy(c, me, second, 1).start()
        d_copy(c, me, partner, 2).start()

    def relay(c):
        d_copy(c, first, partner, 4).wait_recv()
        d_copy(c, first, second, 3).start()
        d_copy(c, first, partner, 4).start()

        @pl.when(c + 3 < NC)
        def _():
            own(c + 3)

    def share(c):
        d_copy(c, second, partner, 5).wait_recv()
        d_copy(c, second, partner, 5).start()
        d_copy(c, dg, partner, 6).wait_recv()
        d_copy(c, dg, partner, 6).start()

    def partner_blocks(c):
        for d in (partner, first + other, second + other, dg + other):
            d_copy(c, d, partner, 0).wait_recv()

    own(0)
    own(1)
    own(2)
    for i in range(ns1):
        w1_copy(i).start()
    for i in range(ns2):
        w2_copy(i).start()

    for j in range(1, DEV):
        s = (me + j) % DEV
        rcopy(lt.at[pl.ds(0, EXP), :], ltr.at[pl.ds(s * EXP, EXP), :], lsend.at[j], lrecv.at[s], s).wait_recv()
    neg = jnp.float32(-jnp.inf)

    def next_max(_, m):
        acc = jnp.full((EXP, TOK), neg, F32)
        for s in range(DEV):
            v = ltr[s * EXP:(s + 1) * EXP, :]
            acc = jnp.maximum(acc, jnp.where(v < m, v, neg))
        return jnp.max(acc, axis=1, keepdims=True)

    t = lax.fori_loop(0, CAP, next_max, jnp.full((EXP, 1), jnp.inf, F32))
    thr_own[...] = jnp.broadcast_to(t, (EXP, 128))
    thr[pl.ds(me * EXP, EXP), :] = jnp.broadcast_to(t, (EXP, 128))

    def t_copy(j, src_dev):
        return rcopy(thr_own, thr.at[pl.ds(src_dev * EXP, EXP), :], tsend.at[j], trecv.at[src_dev], (me + j) % DEV)

    for j in range(1, DEV):
        t_copy(j, me).start()

    relay(0)

    tri = jnp.where(iota((TOK, TOK), 0) < iota((TOK, TOK), 1), 1.0, 0.0).astype(BF16)
    ones = jnp.ones((TOK, TOK), BF16)
    i0, i1 = iota((ALL_EXP, ALL_EXP), 0), iota((ALL_EXP, ALL_EXP), 1)
    s0, e0, s1, e1 = i0 >> 5, i0 & 31, i1 >> 5, i1 & 31
    t8 = jnp.concatenate([t] * DEV, axis=0)
    sel = ltr[...] >= t8
    mo = jnp.where(sel, 1.0, 0.0).astype(BF16)
    cnt = dot(mo, tri)
    num = dot(mo, ones).astype(BF16)
    m_slot = jnp.where((e0 == e1) & (s1 < s0), 1.0, 0.0).astype(BF16)
    m_rank = jnp.where(((s0 >> 1) == (s1 >> 1)) & ((e1 < e0) | ((e1 == e0) & (s1 < s0))), 1.0, 0.0).astype(BF16)
    slot_s[...] = jnp.where(sel, dot(m_slot, num) + cnt, -1.0)
    rank_s[...] = jnp.where(sel, dot(m_rank, num) + cnt, -1.0)

    kio = iota((CAP, TOK), 0).astype(F32)
    lio = iota((CAP, 128), 1)

    def build_p(e, _):
        acc = jnp.zeros((CAP, 128), F32)
        for ch in range(DEV // 2):
            v = jnp.zeros((CAP, TOK), F32)
            for s in (2 * ch, 2 * ch + 1):
                hit = slot_s[pl.ds(s * EXP + e, 1), :] == kio
                p_s[pl.ds(e * CAP, CAP), s * TOK:(s + 1) * TOK] = jnp.where(hit, 1.0, 0.0).astype(BF16)
                v = v + jnp.where(hit, rank_s[pl.ds(s * EXP + e, 1), :] + 1.0, 0.0)
            acc = jnp.where(lio == ch, jnp.sum(v, axis=1, keepdims=True), acc)
        v_s[pl.ds(e * CAP, CAP), :] = acc
        return 0

    lax.fori_loop(0, EXP, build_p, 0, unroll=2)
    relay(1)
    share(0)

    for j in range(1, DEV):
        t_copy(j, (me + j) % DEV).wait_recv()
    la = lt[...]
    sel2 = la >= jnp.concatenate([thr[...], thr[...]], axis=1)
    mt = jnp.where(sel2, 1.0, 0.0).astype(BF16)
    num2 = dot(mt, ones)
    n_own[...] = num2[:, :128]
    n_copy = rcopy(n_own, n_par, nsem.at[0], nsem.at[1], partner)
    n_copy.start()
    ex = jnp.exp(la - jnp.max(la, axis=0, keepdims=True))
    gt_s[...] = ex / jnp.sum(ex, axis=0, keepdims=True)

    relay(2)
    share(1)

    vt_s[...] = v_s[...].T
    rio = iota((bound, SLOTS), 0).astype(F32) + 1.0
    for n, d in enumerate((xn, yn, dg, me)):
        q_s[n * bound:(n + 1) * bound, :] = jnp.where(vt_s[pl.ds(d // 2, 1), :] == rio, 1.0, 0.0).astype(BF16)

    n_copy.wait_recv()
    npar = jnp.concatenate([n_par[...], n_par[...]], axis=1)
    both = num2 + npar
    m_base = jnp.where((s0 == s1) & (e1 < e0), 1.0, 0.0).astype(BF16)
    base = dot(m_base, both.astype(BF16))
    r2_s[...] = jnp.where(sel2, base + dot(mt, tri) + k.astype(F32) * npar, -1.0)
    over = jnp.max(jnp.max(base + both, axis=0, keepdims=True), axis=1, keepdims=True)
    flag_own[...] = jnp.broadcast_to(jnp.where(over > bound, 1.0, 0.0), (8, 128))

    def f_copy(j, src_dev):
        return rcopy(flag_own, flags.at[src_dev], fsend.at[j], frecv.at[src_dev], (me + j) % DEV)

    for j in range(1, DEV):
        f_copy(j, me).start()
    flags[me] = flag_own[...]
    hacc[...] = jnp.zeros((SLOTS, FF), F32)

    def first_product(c, last):
        partner_blocks(c)
        pick_s[...] = dot(p_s[...], xall[c]).astype(BF16)

        def group(g, _):
            i = c * NG + g
            w1_copy(i).wait()
            s = i % ns1
            for j in range(GE):
                rows = pl.ds(g * (GE * CAP) + j * CAP, CAP)
                v = hacc[rows, :] + dot(pick_s[rows, :], w1buf[s, j])
                if last:
                    h_s[rows, :] = gelu(v).astype(BF16)
                else:
                    hacc[rows, :] = v

            @pl.when(i + ns1 < ITEMS)
            def _():
                w1_copy(i + ns1).start()

            return 0

        lax.fori_loop(0, NG, group, 0)

    def chunk(c, _):
        relay(c)
        share(c - 1)
        first_product(c - 2, False)
        return 0

    relay(3)
    share(2)
    first_product(0, False)
    first_product(1, False)
    lax.fori_loop(4, NC, chunk, 0)
    first_product(NC - 2, False)
    share(NC - 1)
    first_product(NC - 1, True)

    def rblk(c, d):
        return recv.at[c, pl.ds(d * bound, bound), :]

    def z_copy(c, n, dev):
        src = rblk(c, me) if n == 3 else zs.at[c, pl.ds(n * bound, bound), :]
        return rcopy(src, rblk(c, me), rsend.at[c * 7 + n], rrecv.at[c * DEV + me], dev)

    def fwd_copy(c, n, block):
        return rcopy(rblk(c, block), rblk(c, block), rsend.at[c * 7 + 4 + n], rrecv.at[c * DEV + block], partner)

    def second_product(c, _):
        def group(g, _):
            i = c * NG + g
            w2_copy(i).wait()
            s = i % ns2
            for j in range(GE):
                rows = pl.ds(g * (GE * CAP) + j * CAP, CAP)
                zc_s[rows, :] = dot(h_s[rows, :], w2buf[s, j]).astype(BF16)

            @pl.when(i + ns2 < ITEMS)
            def _():
                w2_copy(i + ns2).start()

            return 0

        lax.fori_loop(0, NG, group, 0)
        zc = zc_s[...]
        zs[c] = dot(q_s[:3 * bound, :], zc).astype(BF16)
        recv[c, pl.ds(me * bound, bound), :] = dot(q_s[3 * bound:, :], zc).astype(BF16)
        for n, dev in ((2, dg), (0, xn), (1, yn), (3, partner)):
            z_copy(c, n, dev).start()
        return 0

    lax.fori_loop(0, NC, second_product, 0)

    RB = 64

    def build_a(n, _):
        o = n // (bound // RB)
        r0 = (n % (bound // RB)) * RB
        rio2 = (iota((RB, TOK), 0) + r0).astype(F32)

        def one(e, acc):
            row = pl.ds(o * EXP + e, 1)
            return jnp.where(r2_s[row, :] == rio2, gt_s[row, :], acc)

        at_s[pl.ds(o * bound + r0, RB), :] = lax.fori_loop(0, EXP, one, jnp.zeros((RB, TOK), F32), unroll=8)
        return 0

    lax.fori_loop(0, DEV * (bound // RB), build_a, 0)

    def split_a(j, _):
        a = at_s[pl.ds(j * 128, 128), :].T
        for n in range(3):
            part = a.astype(BF16)
            a_s[n, :, pl.ds(j * 128, 128)] = part
            a = a - part.astype(F32)
        return 0

    lax.fori_loop(0, DEV * bound // 128, split_a, 0)

    def forward(c):
        for n, d in enumerate((xn, yn, dg)):
            fwd_copy(c, n, d).wait_recv()
            fwd_copy(c, n, d).start()

    def out_copy(c):
        return pltpu.make_async_copy(out_s.at[c], out.at[:, pl.ds(c * CW, CW)], osem.at[c])

    def combine(c):
        for d in (partner, xn + other, yn + other, dg + other):
            fwd_copy(c, 0, d).wait_recv()
        z = recv[c]
        y = dot(a_s[2], z) + dot(a_s[1], z) + dot(a_s[0], z)
        out_s[c] = (xall[c, pl.ds(me * TOK, TOK), :].astype(F32) + y).astype(BF16)
        out_copy(c).start()

    forward(0)

    def step(c, _):
        forward(c + 1)
        combine(c)
        return 0

    lax.fori_loop(0, NC - 1, step, 0)
    combine(NC - 1)

    acc = flag_own[...]
    for j in range(1, DEV):
        s = (me + j) % DEV
        f_copy(j, s).wait_recv()
        acc = jnp.maximum(acc, flags[s])
    flag_out[...] = acc

    for j in range(1, DEV):
        l_copy(j).wait_send()
        t_copy(j, me).wait_send()
        f_copy(j, me).wait_send()
    n_copy.wait_send()

    def drain(c, _):
        for n, (block, dev) in enumerate(((me, first), (me, second), (me, partner), (first, second),
                                          (first, partner), (second, partner), (dg, partner))):
            d_copy(c, block, dev, n).wait_send()
        for n, dev in enumerate((xn, yn, dg, partner)):
            z_copy(c, n, dev).wait_send()
        for n, d in enumerate((xn, yn, dg)):
            fwd_copy(c, n, d).wait_send()
        out_copy(c).wait()
        return 0

    lax.fori_loop(0, NC, drain, 0)


def moe_call(bound, ns1, ns2, cid, tok, logit, w1, w2):
    vm = pltpu.VMEM
    sem = pltpu.SemaphoreType.DMA
    return pl.pallas_call(
        functools.partial(moe_kernel, bound, ns1, ns2),
        out_shape=(jax.ShapeDtypeStruct((TOK, D), BF16), jax.ShapeDtypeStruct((8, 128), F32)),
        in_specs=[pl.BlockSpec(memory_space=pl.ANY), pl.BlockSpec(memory_space=pl.ANY),
                  pl.BlockSpec(memory_space=pl.ANY), pl.BlockSpec(memory_space=pl.ANY)],
        out_specs=(pl.BlockSpec(memory_space=pl.ANY), pl.BlockSpec(memory_space=pltpu.VMEM)),
        scratch_shapes=[
            vm((NC, DEV * TOK, CW), BF16), vm((ns1, GE, CW, FF), BF16), vm((ns2, GE, FF, CW), BF16),
            vm((TOK, ALL_EXP), F32), vm((ALL_EXP, TOK), F32), vm((ALL_EXP, TOK), F32), vm((EXP, 128), F32), vm((ALL_EXP, 128), F32),
            vm((ALL_EXP, 128), F32), vm((ALL_EXP, 128), F32), vm((8, 128), F32), vm((DEV, 8, 128), F32),
            vm((ALL_EXP, TOK), F32), vm((ALL_EXP, TOK), F32), vm((SLOTS, DEV * TOK), BF16),
            vm((SLOTS, 128), F32), vm((128, SLOTS), F32), vm((4 * bound, SLOTS), BF16),
            vm((SLOTS, CW), BF16), vm((SLOTS, FF), F32), vm((SLOTS, FF), BF16), vm((SLOTS, CW), BF16),
            vm((NC, 3 * bound, CW), BF16), vm((NC, DEV * bound, CW), BF16),
            vm((ALL_EXP, TOK), F32), vm((ALL_EXP, TOK), F32), vm((DEV * bound, TOK), F32),
            vm((3, TOK, DEV * bound), BF16), vm((NC, TOK, CW), BF16),
            sem((ns1,)), sem((ns2,)), sem((NC,)), sem((NC,)), sem((DEV,)), sem((DEV,)), sem((DEV,)), sem((DEV,)),
            sem((DEV,)), sem((DEV,)), sem((3,)), sem((NC * 7,)), sem((NC * DEV,)), sem((NC * 7,)), sem((NC * DEV,)),
        ],
        compiler_params=pltpu.CompilerParams(collective_id=cid, has_side_effects=True, vmem_limit_bytes=67043328),
        name=f"moe_{bound}",
    )(tok, logit, w1, w2)


def solution(mesh):
    row_spec = P(("dp", "ep"), None)
    expert_spec = P("ep", None, None)

    def device_step(tok, logit, w1, w2):
        out, flag = moe_call(192, 5, 8, 0, tok, logit, w1, w2)
        return lax.cond(flag[0, 0] > 0, lambda: moe_call(512, 2, 2, 1, tok, logit, w1, w2)[0], lambda: out)

    return jax.shard_map(device_step, mesh=mesh, in_specs=(row_spec, row_spec, expert_spec, expert_spec),
                         out_specs=row_spec, check_vma=False)
```

```python
import functools

import jax
import jax.numpy as jnp
from jax import lax
from jax.experimental import pallas as pl
from jax.experimental.pallas import tpu as pltpu
from jax.sharding import PartitionSpec as P

MESH = pl.DeviceIdType.MESH
F32, BF16 = jnp.float32, jnp.bfloat16
DEV = 8
TOK = 256
D = 2048
FF = 512
EXP = 32
ALL_EXP = EXP * DEV
CAP = 16
SLOTS = EXP * CAP
NC = 8
CW = D // NC
GE = 8
NG = EXP // GE
ITEMS = NC * NG


def dot(a, b):
    return jnp.dot(a, b, preferred_element_type=F32)


def iota(shape, dim):
    return lax.broadcasted_iota(jnp.int32, shape, dim)


def gelu(v):
    return 0.5 * v * (1.0 + lax.erf(v * 0.7071067811865476))


def dot_nt(a, b):
    return lax.dot_general(a, b, (((1,), (1,)), ((), ())), preferred_element_type=F32)


def onehot(cond):
    return jnp.where(cond, 1.0, 0.0).astype(BF16)


def moe_kernel(xb, nx, bound, ns1, ns2, tok, logit, w1, w2, out, flag_out,
               xr, xs, w1buf, w2buf, log_s, cand, cands, rk, rks, rt_s, w_s, c64_s,
               p_s, v_s, vt_s, q_s, pick_s, hacc, h_s, zc_s, zs, recv,
               r2_s, gt_s, at_s, a_s, out_s,
               w1sem, w2sem, xsem, osem, csend, crecv, ksend, krecv, nsem,
               dsend, drecv, rsend, rrecv):
    me = lax.axis_index("ep")
    k = me % 2
    chip = me // 2
    cx = chip % 2
    cy = chip // 2
    dx = 2 - 4 * cx
    dy = 4 - 8 * cy
    other = 1 - 2 * k
    partner = me + other
    xn, yn, dg = me + dx, me + dy, me + dx + dy
    far = (xn, yn, dg)
    neg = jnp.float32(-jnp.inf)

    def rcopy(src, dst, ss, rs, dev):
        return pltpu.make_async_remote_copy(src_ref=src, dst_ref=dst, send_sem=ss, recv_sem=rs,
                                            device_id={"ep": dev}, device_id_type=MESH)

    def w1_copy(i):
        s = i % ns1
        return pltpu.make_async_copy(
            w1.at[pl.ds((i % NG) * GE, GE), pl.ds((i // NG) * CW, CW), :], w1buf.at[s], w1sem.at[s])

    def w2_copy(i):
        s = i % ns2
        return pltpu.make_async_copy(
            w2.at[pl.ds((i % NG) * GE, GE), :, pl.ds((i // NG) * CW, CW)], w2buf.at[s], w2sem.at[s])

    def xown(c, core):
        return xr.at[c, pl.ds(core * TOK, TOK), :]

    def xlist(c, n, core):
        return xr.at[c, pl.ds(2 * TOK + (2 * n + core) * xb, xb), :]

    def x_copy(c):
        return pltpu.make_async_copy(tok.at[:, pl.ds(c * CW, CW)], xown(c, k), xsem.at[c])

    def p_copy(c, core):
        return rcopy(xown(c, core), xown(c, core), dsend.at[c * 7 + 6], drecv.at[c * DEV + 6], partner)

    def x_send(c, n):
        return rcopy(xs.at[c, pl.ds(n * xb, xb), :], xlist(c, n, k), dsend.at[c * 7 + n],
                     drecv.at[c * DEV + 2 * n + k], far[n])

    def x_fwd(c, n, core):
        return rcopy(xlist(c, n, core), xlist(c, n, core), dsend.at[c * 7 + 3 + n],
                     drecv.at[c * DEV + 2 * n + core], partner)

    barrier = pltpu.get_barrier_semaphore()
    for j in range(1, DEV):
        pl.semaphore_signal(barrier, inc=1, device_id={"ep": (me + j) % DEV}, device_id_type=MESH)
    log_copy = pltpu.make_async_copy(logit, log_s, nsem.at[0])
    log_copy.start()
    for c in range(NC):
        x_copy(c).start()
    log_copy.wait()

    def next_top(n, m):
        v = log_s[...]
        m = jnp.max(jnp.where(v < m, v, neg), axis=0, keepdims=True)
        cand[pl.ds(n, 1), :] = m
        return m

    lax.fori_loop(0, 8, next_top, jnp.full((1, ALL_EXP), jnp.inf, F32))
    pl.semaphore_wait(barrier, DEV - 1)

    def c_copy(j, src):
        return rcopy(cand, cands.at[pl.ds(src * 8, 8), :], csend.at[j], crecv.at[src], (me + j) % DEV)

    def k_copy(j, src):
        return rcopy(rk, rks.at[pl.ds(src * 8, 8), :], ksend.at[j], krecv.at[src], (me + j) % DEV)

    for j in range(1, DEV):
        c_copy(j, me).start()
    cands[pl.ds(me * 8, 8), :] = cand[...]

    def start_own(c, _):
        x_copy(c).wait()
        p_copy(c, k).start()
        return 0

    lax.fori_loop(0, NC, start_own, 0)
    if nx > 2 * TOK + 6 * xb:
        for c in range(NC):
            xr[c, 2 * TOK + 6 * xb:, :] = jnp.zeros((nx - 2 * TOK - 6 * xb, CW), BF16)
    t0, t1 = iota((TOK, TOK), 0), iota((TOK, TOK), 1)
    tri = onehot(t0 < t1)
    for j in range(1, DEV):
        c_copy(j, (me + j) % DEV).wait_recv()

    def next_max(_, m):
        v = cands[...]
        return jnp.max(jnp.where(v < m, v, neg), axis=0, keepdims=True)

    thr = lax.fori_loop(0, CAP, next_max, jnp.full((1, ALL_EXP), jnp.inf, F32))

    mo = onehot(log_s[...] >= thr)
    of_chip = onehot((iota((16, ALL_EXP), 1) >> 6) == iota((16, ALL_EXP), 0))
    used = dot_nt(of_chip, mo) > 0.5
    rt_s[...] = jnp.where(used, dot(onehot(used), tri), -1.0)
    xio = iota((xb, TOK), 0).astype(F32)
    for n in range(3):
        w_s[n * xb:(n + 1) * xb, :] = onehot(rt_s[pl.ds(far[n] // 2, 1), :] == xio)

    def compact(c, _):
        xs[c] = dot(w_s[...], xr[c, pl.ds(k * TOK, TOK), :]).astype(BF16)
        for n in (2, 0, 1):
            x_send(c, n).start()
        return 0

    lax.fori_loop(0, NC, compact, 0)
    for i in range(ns1):
        w1_copy(i).start()
    for i in range(ns2):
        w2_copy(i).start()

    of_chip2 = onehot((iota((ALL_EXP, 128), 0) >> 6) == iota((ALL_EXP, 128), 1))
    used2 = onehot(dot(mo, of_chip2) > 0.5)
    place = dot(onehot(t1 < t0), used2)
    place = jnp.where(iota((TOK, 128), 1) == chip, iota((TOK, 128), 0).astype(F32), place)
    place = dot_nt(place.astype(BF16), of_chip2)
    c64_s[...] = place

    def top_place(n, _):
        hit = log_s[...] == cand[pl.ds(n, 1), :]
        rk[pl.ds(n, 1), :] = jnp.max(jnp.where(hit, c64_s[...], -1.0), axis=0, keepdims=True)
        return 0

    lax.fori_loop(0, 8, top_place, 0)
    for j in range(1, DEV):
        k_copy(j, me).start()
    rks[pl.ds(me * 8, 8), :] = rk[...]

    cv = cands[...]
    sel = cv >= thr
    so = onehot(sel)
    j0, j1 = iota((64, 64), 0), iota((64, 64), 1)
    slot = dot(onehot(j1 < j0), so)
    inside = dot(onehot((j1 < j0) & ((j1 >> 4) == (j0 >> 4))), so)
    num = dot(onehot((j1 >> 4) == (j0 >> 4)), so)
    base = dot(num.astype(BF16), onehot((t0 < t1) & ((t0 >> 5) == (t1 >> 5))))
    rank = base + inside
    over = jnp.max(jnp.max(base + num, axis=0, keepdims=True), axis=1, keepdims=True) > bound
    c64_s[:64, :] = jnp.where(sel, rank, -1.0)

    pair = jnp.full((TOK, ALL_EXP), -1.0, F32)
    for n in range(8):
        pair = jnp.where(log_s[...] == cand[n:n + 1, :], c64_s[pl.ds(me * 8 + n, 1), :], pair)
    r2_s[...] = pair.T
    la = log_s[...].T
    ex = jnp.exp(la - jnp.max(la, axis=0, keepdims=True))
    gt_s[...] = ex / jnp.sum(ex, axis=0, keepdims=True)

    for j in range(1, DEV):
        k_copy(j, (me + j) % DEV).wait_recv()
    rv = rks[...]
    src = iota((64, ALL_EXP), 0) >> 3
    exp_chip = iota((64, ALL_EXP), 1) >> 6
    wide = jnp.max(jnp.max(jnp.where(sel & ((src >> 1) != exp_chip), rv, -1.0), axis=0, keepdims=True),
                   axis=1, keepdims=True) >= xb
    flag_out[...] = jnp.broadcast_to(jnp.where(over | wide, 1.0, 0.0), (8, 128))
    rel = (src >> 1) ^ chip
    start = jnp.where(rel == 0, (src & 1) * TOK, 2 * TOK + (2 * (rel - 1) + (src & 1)) * xb).astype(F32)
    pos = start + rv + 1.0
    code = ((src >> 1) * 1024).astype(F32) + rank + 1.0
    pos_rows, code_rows = [], []
    for i in range(CAP):
        hit = sel & (slot == i)
        pos_rows.append(jnp.sum(jnp.where(hit, pos, 0.0), axis=0, keepdims=True))
        code_rows.append(jnp.sum(jnp.where(hit, code, 0.0), axis=0, keepdims=True))
    turn = ALL_EXP - me * EXP
    pos = pltpu.roll(jnp.concatenate(pos_rows, axis=0), turn, 1)
    code = pltpu.roll(jnp.concatenate(code_rows, axis=0), turn, 1)
    pio = iota((CAP, nx), 1).astype(F32) + 1.0
    for e in range(EXP):
        p_s[e * CAP:(e + 1) * CAP, :] = onehot(pos[:, e:e + 1] == pio)
        v_s[e * CAP:(e + 1) * CAP, :] = jnp.broadcast_to(code[:, e:e + 1], (CAP, 128))
    vt_s[...] = v_s[...].T[:8, :]
    rio = iota((bound, SLOTS), 0)
    for n, d in enumerate((xn, yn, dg, me)):
        want = (rio + ((d // 2) * 1024 + 1)).astype(F32)
        q_s[n * bound:(n + 1) * bound, :] = onehot(vt_s[0:1, :] == want)
    hacc[...] = jnp.zeros((SLOTS, FF), F32)

    def x_forward(c):
        for n in range(3):
            x_fwd(c, n, k).wait_recv()
            x_fwd(c, n, k).start()

    def first_product(c, last):
        for n in range(3):
            x_fwd(c, n, 1 - k).wait_recv()
        p_copy(c, 1 - k).wait_recv()
        pick_s[...] = dot(p_s[...], xr[c]).astype(BF16)

        def group(g, _):
            i = c * NG + g
            w1_copy(i).wait()
            s = i % ns1
            for j in range(GE):
                rows = pl.ds(g * (GE * CAP) + j * CAP, CAP)
                v = hacc[rows, :] + dot(pick_s[rows, :], w1buf[s, j])
                if last:
                    h_s[rows, :] = gelu(v).astype(BF16)
                else:
                    hacc[rows, :] = v

            @pl.when(i + ns1 < ITEMS)
            def _():
                w1_copy(i + ns1).start()

            return 0

        lax.fori_loop(0, NG, group, 0)

    def chunk(c, _):
        x_forward(c + 1)
        first_product(c, False)
        return 0

    x_forward(0)
    lax.fori_loop(0, NC - 1, chunk, 0)
    first_product(NC - 1, True)

    def rblk(c, d):
        return recv.at[c, pl.ds(d * bound, bound), :]

    def z_copy(c, n, dev):
        src = rblk(c, me) if n == 3 else zs.at[c, pl.ds(n * bound, bound), :]
        return rcopy(src, rblk(c, me), rsend.at[c * 7 + n], rrecv.at[c * DEV + me], dev)

    def fwd_copy(c, n, block):
        return rcopy(rblk(c, block), rblk(c, block), rsend.at[c * 7 + 4 + n], rrecv.at[c * DEV + block], partner)

    def second_product(c, _):
        def group(g, _):
            i = c * NG + g
            w2_copy(i).wait()
            s = i % ns2
            for j in range(GE):
                rows = pl.ds(g * (GE * CAP) + j * CAP, CAP)
                zc_s[rows, :] = dot(h_s[rows, :], w2buf[s, j]).astype(BF16)

            @pl.when(i + ns2 < ITEMS)
            def _():
                w2_copy(i + ns2).start()

            return 0

        lax.fori_loop(0, NG, group, 0)
        zc = zc_s[...]
        zs[c] = dot(q_s[:3 * bound, :], zc).astype(BF16)
        recv[c, pl.ds(me * bound, bound), :] = dot(q_s[3 * bound:, :], zc).astype(BF16)
        for n, dev in ((2, dg), (0, xn), (1, yn), (3, partner)):
            z_copy(c, n, dev).start()
        return 0

    lax.fori_loop(0, NC, second_product, 0)

    RB = 64

    def build_a(n, _):
        o = n // (bound // RB)
        r0 = (n % (bound // RB)) * RB
        rio2 = (iota((RB, TOK), 0) + r0).astype(F32)

        def one(e, acc):
            row = pl.ds(o * EXP + e, 1)
            return jnp.where(r2_s[row, :] == rio2, gt_s[row, :], acc)

        at_s[pl.ds(o * bound + r0, RB), :] = lax.fori_loop(0, EXP, one, jnp.zeros((RB, TOK), F32), unroll=8)
        return 0

    lax.fori_loop(0, DEV * (bound // RB), build_a, 0)

    def split_a(j, _):
        a = at_s[pl.ds(j * 128, 128), :].T
        for n in range(3):
            part = a.astype(BF16)
            a_s[n, :, pl.ds(j * 128, 128)] = part
            a = a - part.astype(F32)
        return 0

    lax.fori_loop(0, DEV * bound // 128, split_a, 0)

    def forward(c):
        for n, d in enumerate((xn, yn, dg)):
            fwd_copy(c, n, d).wait_recv()
            fwd_copy(c, n, d).start()

    def out_copy(c):
        return pltpu.make_async_copy(out_s.at[c], out.at[:, pl.ds(c * CW, CW)], osem.at[c])

    def combine(c):
        for d in (partner, xn + other, yn + other, dg + other):
            fwd_copy(c, 0, d).wait_recv()
        z = recv[c]
        y = dot(a_s[2], z) + dot(a_s[1], z) + dot(a_s[0], z)
        out_s[c] = (xr[c, pl.ds(k * TOK, TOK), :].astype(F32) + y).astype(BF16)
        out_copy(c).start()

    forward(0)

    def step(c, _):
        forward(c + 1)
        combine(c)
        return 0

    lax.fori_loop(0, NC - 1, step, 0)
    combine(NC - 1)

    for j in range(1, DEV):
        c_copy(j, me).wait_send()
        k_copy(j, me).wait_send()

    def drain(c, _):
        p_copy(c, k).wait_send()
        for n in range(3):
            x_send(c, n).wait_send()
            x_fwd(c, n, k).wait_send()
        for n, dev in enumerate((xn, yn, dg, partner)):
            z_copy(c, n, dev).wait_send()
        for n, d in enumerate((xn, yn, dg)):
            fwd_copy(c, n, d).wait_send()
        out_copy(c).wait()
        return 0

    lax.fori_loop(0, NC, drain, 0)


def moe_call(xb, bound, ns1, ns2, cid, tok, logit, w1, w2):
    nx = -(-(2 * TOK + 6 * xb) // 128) * 128
    vm = pltpu.VMEM
    sem = pltpu.SemaphoreType.DMA
    sq = vm((ALL_EXP, TOK), F32)
    return pl.pallas_call(
        functools.partial(moe_kernel, xb, nx, bound, ns1, ns2),
        out_shape=(jax.ShapeDtypeStruct((TOK, D), BF16), jax.ShapeDtypeStruct((8, 128), F32)),
        in_specs=[pl.BlockSpec(memory_space=pl.ANY)] * 4,
        out_specs=(pl.BlockSpec(memory_space=pl.ANY), pl.BlockSpec(memory_space=pltpu.VMEM)),
        scratch_shapes=[
            vm((NC, nx, CW), BF16), vm((NC, 3 * xb, CW), BF16),
            vm((ns1, GE, CW, FF), BF16), vm((ns2, GE, FF, CW), BF16),
            sq, vm((8, ALL_EXP), F32), vm((64, ALL_EXP), F32), vm((8, ALL_EXP), F32), vm((64, ALL_EXP), F32),
            vm((16, TOK), F32), vm((3 * xb, TOK), BF16), sq,
            vm((SLOTS, nx), BF16), vm((SLOTS, 128), F32), vm((8, SLOTS), F32), vm((4 * bound, SLOTS), BF16),
            vm((SLOTS, CW), BF16), vm((SLOTS, FF), F32), vm((SLOTS, FF), BF16), vm((SLOTS, CW), BF16),
            vm((NC, 3 * bound, CW), BF16), vm((NC, DEV * bound, CW), BF16),
            sq, sq, vm((DEV * bound, TOK), F32), vm((3, TOK, DEV * bound), BF16), vm((NC, TOK, CW), BF16),
            sem((ns1,)), sem((ns2,)), sem((NC,)), sem((NC,)), sem((DEV,)), sem((DEV,)), sem((DEV,)), sem((DEV,)),
            sem((1,)), sem((NC * 7,)), sem((NC * DEV,)), sem((NC * 7,)), sem((NC * DEV,)),
        ],
        compiler_params=pltpu.CompilerParams(collective_id=cid, has_side_effects=True, vmem_limit_bytes=67043328),
        name=f"moe_{bound}",
    )(tok, logit, w1, w2)


def solution(mesh):
    row_spec = P(("dp", "ep"), None)
    expert_spec = P("ep", None, None)

    def device_step(tok, logit, w1, w2):
        out, flag = moe_call(144, 192, 5, 8, 0, tok, logit, w1, w2)
        return lax.cond(flag[0, 0] > 0, lambda: moe_call(TOK, 512, 2, 2, 1, tok, logit, w1, w2)[0], lambda: out)

    return jax.shard_map(device_step, mesh=mesh, in_specs=(row_spec, row_spec, expert_spec, expert_spec),
                         out_specs=row_spec, check_vma=False)
```

```python
import functools

import jax
import jax.numpy as jnp
from jax import lax
from jax.experimental import pallas as pl
from jax.experimental.pallas import tpu as pltpu
from jax.sharding import PartitionSpec as P

MESH = pl.DeviceIdType.MESH
F32, BF16 = jnp.float32, jnp.bfloat16
DEV = 8
TOK = 256
D = 2048
FF = 512
EXP = 32
ALL_EXP = EXP * DEV
CAP = 16
SLOTS = EXP * CAP
NC = 8
CW = D // NC
GE = 8
NG = EXP // GE
ITEMS = NC * NG


def dot(a, b):
    return jnp.dot(a, b, preferred_element_type=F32)


def iota(shape, dim):
    return lax.broadcasted_iota(jnp.int32, shape, dim)


def gelu(v):
    return 0.5 * v * (1.0 + lax.erf(v * 0.7071067811865476))


def dot_nt(a, b):
    return lax.dot_general(a, b, (((1,), (1,)), ((), ())), preferred_element_type=F32)


def onehot(cond):
    return jnp.where(cond, 1.0, 0.0).astype(BF16)


def moe_kernel(xb, nx, bound, ns1, ns2, tok, logit, w1, w2, out, flag_out,
               xr, xs, w1buf, w2buf, log_s, cand, cands, rk, rks, rt_s, w_s, c64_s,
               p_s, v_s, vt_s, q_s, pick_s, hacc, h_s, zc_s, zs, recv,
               r2_s, gt_s, at_s, a_s, out_s,
               w1sem, w2sem, xsem, osem, csend, crecv, ksend, krecv, nsem,
               dsend, drecv, rsend, rrecv):
    me = lax.axis_index("ep")
    k = me % 2
    chip = me // 2
    cx = chip % 2
    cy = chip // 2
    dx = 2 - 4 * cx
    dy = 4 - 8 * cy
    other = 1 - 2 * k
    partner = me + other
    xn, yn, dg = me + dx, me + dy, me + dx + dy
    far = (xn, yn, dg)
    neg = jnp.float32(-jnp.inf)

    def rcopy(src, dst, ss, rs, dev):
        return pltpu.make_async_remote_copy(src_ref=src, dst_ref=dst, send_sem=ss, recv_sem=rs,
                                            device_id={"ep": dev}, device_id_type=MESH)

    def w1_copy(i):
        s = i % ns1
        return pltpu.make_async_copy(
            w1.at[pl.ds((i % NG) * GE, GE), pl.ds((i // NG) * CW, CW), :], w1buf.at[s], w1sem.at[s])

    def w2_copy(i):
        s = i % ns2
        return pltpu.make_async_copy(
            w2.at[pl.ds((i % NG) * GE, GE), :, pl.ds((i // NG) * CW, CW)], w2buf.at[s], w2sem.at[s])

    def xown(c, core):
        return xr.at[c, pl.ds(core * TOK, TOK), :]

    def xlist(c, n, core):
        return xr.at[c, pl.ds(2 * TOK + (2 * n + core) * xb, xb), :]

    def x_copy(c):
        return pltpu.make_async_copy(tok.at[:, pl.ds(c * CW, CW)], xown(c, k), xsem.at[c])

    def p_copy(c, core):
        return rcopy(xown(c, core), xown(c, core), dsend.at[c * 7 + 6], drecv.at[c * DEV + 6], partner)

    def x_send(c, n):
        return rcopy(xs.at[c, pl.ds(n * xb, xb), :], xlist(c, n, k), dsend.at[c * 7 + n],
                     drecv.at[c * DEV + 2 * n + k], far[n])

    def x_fwd(c, n, core):
        return rcopy(xlist(c, n, core), xlist(c, n, core), dsend.at[c * 7 + 3 + n],
                     drecv.at[c * DEV + 2 * n + core], partner)

    barrier = pltpu.get_barrier_semaphore()
    for j in range(1, DEV):
        pl.semaphore_signal(barrier, inc=1, device_id={"ep": (me + j) % DEV}, device_id_type=MESH)
    log_copy = pltpu.make_async_copy(logit, log_s, nsem.at[0])
    log_copy.start()
    for c in range(NC):
        x_copy(c).start()
    log_copy.wait()

    def next_top(n, m):
        v = log_s[...]
        m = jnp.max(jnp.where(v < m, v, neg), axis=0, keepdims=True)
        cand[pl.ds(n, 1), :] = m
        return m

    lax.fori_loop(0, 8, next_top, jnp.full((1, ALL_EXP), jnp.inf, F32))
    pl.semaphore_wait(barrier, DEV - 1)

    def c_copy(j, src):
        return rcopy(cand, cands.at[pl.ds(src * 8, 8), :], csend.at[j], crecv.at[src], (me + j) % DEV)

    def k_copy(j, src):
        return rcopy(rk, rks.at[pl.ds(src * 8, 8), :], ksend.at[j], krecv.at[src], (me + j) % DEV)

    for j in range(1, DEV):
        c_copy(j, me).start()
    cands[pl.ds(me * 8, 8), :] = cand[...]

    def start_own(c, _):
        x_copy(c).wait()
        p_copy(c, k).start()
        return 0

    lax.fori_loop(0, NC, start_own, 0)
    if nx > 2 * TOK + 6 * xb:
        for c in range(NC):
            xr[c, 2 * TOK + 6 * xb:, :] = jnp.zeros((nx - 2 * TOK - 6 * xb, CW), BF16)
    t0, t1 = iota((TOK, TOK), 0), iota((TOK, TOK), 1)
    tri = onehot(t0 < t1)
    for j in range(1, DEV):
        c_copy(j, (me + j) % DEV).wait_recv()

    def next_max(_, m):
        v = cands[...]
        return jnp.max(jnp.where(v < m, v, neg), axis=0, keepdims=True)

    thr = lax.fori_loop(0, CAP, next_max, jnp.full((1, ALL_EXP), jnp.inf, F32))

    mo = onehot(log_s[...] >= thr)
    of_chip = onehot((iota((16, ALL_EXP), 1) >> 6) == iota((16, ALL_EXP), 0))
    used = dot_nt(of_chip, mo) > 0.5
    rt_s[...] = jnp.where(used, dot(onehot(used), tri), -1.0)
    xio = iota((xb, TOK), 0).astype(F32)
    for n in range(3):
        w_s[n * xb:(n + 1) * xb, :] = onehot(rt_s[pl.ds(far[n] // 2, 1), :] == xio)

    def compact(c, _):
        xs[c] = dot(w_s[...], xr[c, pl.ds(k * TOK, TOK), :]).astype(BF16)
        for n in (2, 0, 1):
            x_send(c, n).start()
        return 0

    compact(0, 0)

    of_chip2 = onehot((iota((ALL_EXP, 128), 0) >> 6) == iota((ALL_EXP, 128), 1))
    used2 = onehot(dot(mo, of_chip2) > 0.5)
    place = dot(onehot(t1 < t0), used2)
    place = jnp.where(iota((TOK, 128), 1) == chip, iota((TOK, 128), 0).astype(F32), place)
    place = dot_nt(place.astype(BF16), of_chip2)
    c64_s[...] = place

    def top_place(n, _):
        hit = log_s[...] == cand[pl.ds(n, 1), :]
        rk[pl.ds(n, 1), :] = jnp.max(jnp.where(hit, c64_s[...], -1.0), axis=0, keepdims=True)
        return 0

    lax.fori_loop(0, 8, top_place, 0)
    for j in range(1, DEV):
        k_copy(j, me).start()
    rks[pl.ds(me * 8, 8), :] = rk[...]
    lax.fori_loop(1, NC, compact, 0)
    for i in range(ns1):
        w1_copy(i).start()
    for i in range(ns2):
        w2_copy(i).start()

    cv = cands[...]
    sel = cv >= thr
    so = onehot(sel)
    j0, j1 = iota((64, 64), 0), iota((64, 64), 1)
    slot = dot(onehot(j1 < j0), so)
    inside = dot(onehot((j1 < j0) & ((j1 >> 4) == (j0 >> 4))), so)
    num = dot(onehot((j1 >> 4) == (j0 >> 4)), so)
    base = dot(num.astype(BF16), onehot((t0 < t1) & ((t0 >> 5) == (t1 >> 5))))
    rank = base + inside
    over = jnp.max(jnp.max(base + num, axis=0, keepdims=True), axis=1, keepdims=True) > bound
    c64_s[:64, :] = jnp.where(sel, rank, -1.0)

    pair = jnp.full((TOK, ALL_EXP), -1.0, F32)
    for n in range(8):
        pair = jnp.where(log_s[...] == cand[n:n + 1, :], c64_s[pl.ds(me * 8 + n, 1), :], pair)
    r2_s[...] = pair.T
    la = log_s[...].T
    ex = jnp.exp(la - jnp.max(la, axis=0, keepdims=True))
    gt_s[...] = ex / jnp.sum(ex, axis=0, keepdims=True)

    for j in range(1, DEV):
        k_copy(j, (me + j) % DEV).wait_recv()
    rv = rks[...]
    src = iota((64, ALL_EXP), 0) >> 3
    exp_chip = iota((64, ALL_EXP), 1) >> 6
    wide = jnp.max(jnp.max(jnp.where(sel & ((src >> 1) != exp_chip), rv, -1.0), axis=0, keepdims=True),
                   axis=1, keepdims=True) >= xb
    flag_out[...] = jnp.broadcast_to(jnp.where(over | wide, 1.0, 0.0), (8, 128))
    rel = (src >> 1) ^ chip
    start = jnp.where(rel == 0, (src & 1) * TOK, 2 * TOK + (2 * (rel - 1) + (src & 1)) * xb).astype(F32)
    pos = start + rv + 1.0
    code = ((src >> 1) * 1024).astype(F32) + rank + 1.0
    pos_rows, code_rows = [], []
    for i in range(CAP):
        hit = sel & (slot == i)
        pos_rows.append(jnp.sum(jnp.where(hit, pos, 0.0), axis=0, keepdims=True))
        code_rows.append(jnp.sum(jnp.where(hit, code, 0.0), axis=0, keepdims=True))
    turn = ALL_EXP - me * EXP
    pos = pltpu.roll(jnp.concatenate(pos_rows, axis=0), turn, 1)
    code = pltpu.roll(jnp.concatenate(code_rows, axis=0), turn, 1)
    pio = iota((CAP, nx), 1).astype(F32) + 1.0
    for e in range(EXP):
        p_s[e * CAP:(e + 1) * CAP, :] = onehot(pos[:, e:e + 1] == pio)
        v_s[e * CAP:(e + 1) * CAP, :] = jnp.broadcast_to(code[:, e:e + 1], (CAP, 128))
    vt_s[...] = v_s[...].T[:8, :]
    rio = iota((bound, SLOTS), 0)
    for n, d in enumerate((xn, yn, dg, me)):
        want = (rio + ((d // 2) * 1024 + 1)).astype(F32)
        q_s[n * bound:(n + 1) * bound, :] = onehot(vt_s[0:1, :] == want)
    hacc[...] = jnp.zeros((SLOTS, FF), F32)

    def x_forward(c):
        for n in range(3):
            x_fwd(c, n, k).wait_recv()
            x_fwd(c, n, k).start()

    def first_product(c, last):
        for n in range(3):
            x_fwd(c, n, 1 - k).wait_recv()
        p_copy(c, 1 - k).wait_recv()
        pick_s[...] = dot(p_s[...], xr[c]).astype(BF16)

        def group(g, _):
            i = c * NG + g
            w1_copy(i).wait()
            s = i % ns1
            for j in range(GE):
                rows = pl.ds(g * (GE * CAP) + j * CAP, CAP)
                v = hacc[rows, :] + dot(pick_s[rows, :], w1buf[s, j])
                if last:
                    h_s[rows, :] = gelu(v).astype(BF16)
                else:
                    hacc[rows, :] = v

            @pl.when(i + ns1 < ITEMS)
            def _():
                w1_copy(i + ns1).start()

            return 0

        lax.fori_loop(0, NG, group, 0)

    def chunk(c, _):
        x_forward(c + 1)
        first_product(c, False)
        return 0

    x_forward(0)
    lax.fori_loop(0, NC - 1, chunk, 0)
    first_product(NC - 1, True)

    def rblk(c, d):
        return recv.at[c, pl.ds(d * bound, bound), :]

    def z_copy(c, n, dev):
        src = rblk(c, me) if n == 3 else zs.at[c, pl.ds(n * bound, bound), :]
        return rcopy(src, rblk(c, me), rsend.at[c * 7 + n], rrecv.at[c * DEV + me], dev)

    def fwd_copy(c, n, block):
        return rcopy(rblk(c, block), rblk(c, block), rsend.at[c * 7 + 4 + n], rrecv.at[c * DEV + block], partner)

    def second_product(c, _):
        def group(g, _):
            i = c * NG + g
            w2_copy(i).wait()
            s = i % ns2
            for j in range(GE):
                rows = pl.ds(g * (GE * CAP) + j * CAP, CAP)
                zc_s[rows, :] = dot(h_s[rows, :], w2buf[s, j]).astype(BF16)

            @pl.when(i + ns2 < ITEMS)
            def _():
                w2_copy(i + ns2).start()

            return 0

        lax.fori_loop(0, NG, group, 0)
        zc = zc_s[...]
        zs[c] = dot(q_s[:3 * bound, :], zc).astype(BF16)
        recv[c, pl.ds(me * bound, bound), :] = dot(q_s[3 * bound:, :], zc).astype(BF16)
        for n, dev in ((2, dg), (0, xn), (1, yn), (3, partner)):
            z_copy(c, n, dev).start()
        return 0

    lax.fori_loop(0, NC, second_product, 0)

    RB = 64

    def build_a(n, _):
        o = n // (bound // RB)
        r0 = (n % (bound // RB)) * RB
        rio2 = (iota((RB, TOK), 0) + r0).astype(F32)

        def one(e, acc):
            row = pl.ds(o * EXP + e, 1)
            return jnp.where(r2_s[row, :] == rio2, gt_s[row, :], acc)

        at_s[pl.ds(o * bound + r0, RB), :] = lax.fori_loop(0, EXP, one, jnp.zeros((RB, TOK), F32), unroll=8)
        return 0

    lax.fori_loop(0, DEV * (bound // RB), build_a, 0)

    def split_a(j, _):
        a = at_s[pl.ds(j * 128, 128), :].T
        for n in range(3):
            part = a.astype(BF16)
            a_s[n, :, pl.ds(j * 128, 128)] = part
            a = a - part.astype(F32)
        return 0

    lax.fori_loop(0, DEV * bound // 128, split_a, 0)

    def forward(c):
        for n, d in enumerate((xn, yn, dg)):
            fwd_copy(c, n, d).wait_recv()
            fwd_copy(c, n, d).start()

    def out_copy(c):
        return pltpu.make_async_copy(out_s.at[c], out.at[:, pl.ds(c * CW, CW)], osem.at[c])

    def combine(c):
        for d in (partner, xn + other, yn + other, dg + other):
            fwd_copy(c, 0, d).wait_recv()
        z = recv[c]
        y = dot(a_s[2], z) + dot(a_s[1], z) + dot(a_s[0], z)
        out_s[c] = (xr[c, pl.ds(k * TOK, TOK), :].astype(F32) + y).astype(BF16)
        out_copy(c).start()

    forward(0)

    def step(c, _):
        forward(c + 1)
        combine(c)
        return 0

    lax.fori_loop(0, NC - 1, step, 0)
    combine(NC - 1)

    for j in range(1, DEV):
        c_copy(j, me).wait_send()
        k_copy(j, me).wait_send()

    def drain(c, _):
        p_copy(c, k).wait_send()
        for n in range(3):
            x_send(c, n).wait_send()
            x_fwd(c, n, k).wait_send()
        for n, dev in enumerate((xn, yn, dg, partner)):
            z_copy(c, n, dev).wait_send()
        for n, d in enumerate((xn, yn, dg)):
            fwd_copy(c, n, d).wait_send()
        out_copy(c).wait()
        return 0

    lax.fori_loop(0, NC, drain, 0)


def moe_call(xb, bound, ns1, ns2, cid, tok, logit, w1, w2):
    nx = -(-(2 * TOK + 6 * xb) // 128) * 128
    vm = pltpu.VMEM
    sem = pltpu.SemaphoreType.DMA
    sq = vm((ALL_EXP, TOK), F32)
    return pl.pallas_call(
        functools.partial(moe_kernel, xb, nx, bound, ns1, ns2),
        out_shape=(jax.ShapeDtypeStruct((TOK, D), BF16), jax.ShapeDtypeStruct((8, 128), F32)),
        in_specs=[pl.BlockSpec(memory_space=pl.ANY)] * 4,
        out_specs=(pl.BlockSpec(memory_space=pl.ANY), pl.BlockSpec(memory_space=pltpu.VMEM)),
        scratch_shapes=[
            vm((NC, nx, CW), BF16), vm((NC, 3 * xb, CW), BF16),
            vm((ns1, GE, CW, FF), BF16), vm((ns2, GE, FF, CW), BF16),
            sq, vm((8, ALL_EXP), F32), vm((64, ALL_EXP), F32), vm((8, ALL_EXP), F32), vm((64, ALL_EXP), F32),
            vm((16, TOK), F32), vm((3 * xb, TOK), BF16), sq,
            vm((SLOTS, nx), BF16), vm((SLOTS, 128), F32), vm((8, SLOTS), F32), vm((4 * bound, SLOTS), BF16),
            vm((SLOTS, CW), BF16), vm((SLOTS, FF), F32), vm((SLOTS, FF), BF16), vm((SLOTS, CW), BF16),
            vm((NC, 3 * bound, CW), BF16), vm((NC, DEV * bound, CW), BF16),
            sq, sq, vm((DEV * bound, TOK), F32), vm((3, TOK, DEV * bound), BF16), vm((NC, TOK, CW), BF16),
            sem((ns1,)), sem((ns2,)), sem((NC,)), sem((NC,)), sem((DEV,)), sem((DEV,)), sem((DEV,)), sem((DEV,)),
            sem((1,)), sem((NC * 7,)), sem((NC * DEV,)), sem((NC * 7,)), sem((NC * DEV,)),
        ],
        compiler_params=pltpu.CompilerParams(collective_id=cid, has_side_effects=True, vmem_limit_bytes=67043328),
        name=f"moe_{bound}",
    )(tok, logit, w1, w2)


def solution(mesh):
    row_spec = P(("dp", "ep"), None)
    expert_spec = P("ep", None, None)

    def device_step(tok, logit, w1, w2):
        out, flag = moe_call(144, 192, 5, 8, 0, tok, logit, w1, w2)
        return lax.cond(flag[0, 0] > 0, lambda: moe_call(TOK, 512, 2, 2, 1, tok, logit, w1, w2)[0], lambda: out)

    return jax.shard_map(device_step, mesh=mesh, in_specs=(row_spec, row_spec, expert_spec, expert_spec),
                         out_specs=row_spec, check_vma=False)
```

```python
import functools

import jax
import jax.numpy as jnp
from jax import lax
from jax.experimental import pallas as pl
from jax.experimental.pallas import tpu as pltpu
from jax.sharding import PartitionSpec as P

MESH = pl.DeviceIdType.MESH
F32, BF16 = jnp.float32, jnp.bfloat16
DEV = 8
TOK = 256
D = 2048
FF = 512
EXP = 32
ALL_EXP = EXP * DEV
CAP = 16
SLOTS = EXP * CAP
NC = 8
CW = D // NC
GE = 8
NG = EXP // GE
ITEMS = NC * NG


def dot(a, b):
    return jnp.dot(a, b, preferred_element_type=F32)


def iota(shape, dim):
    return lax.broadcasted_iota(jnp.int32, shape, dim)


def gelu(v):
    return 0.5 * v * (1.0 + lax.erf(v * 0.7071067811865476))


def dot_nt(a, b):
    return lax.dot_general(a, b, (((1,), (1,)), ((), ())), preferred_element_type=F32)


def onehot(cond):
    return jnp.where(cond, 1.0, 0.0).astype(BF16)


def moe_kernel(xb, nx, bound, ns1, ns2, tok, logit, w1, w2, out, flag_out,
               xr, xs, w1buf, w2buf, log_s, cand, cands, rk, rks, rt_s, w_s, c64_s,
               p_s, v_s, vt_s, q_s, pick_s, hacc, h_s, zc_s, zs, recv,
               r2_s, gt_s, at_s, a_s, out_s,
               w1sem, w2sem, xsem, osem, csend, crecv, ksend, krecv, nsem,
               dsend, drecv, rsend, rrecv):
    me = lax.axis_index("ep")
    k = me % 2
    chip = me // 2
    cx = chip % 2
    cy = chip // 2
    dx = 2 - 4 * cx
    dy = 4 - 8 * cy
    other = 1 - 2 * k
    partner = me + other
    xn, yn, dg = me + dx, me + dy, me + dx + dy
    far = (xn, yn, dg)
    neg = jnp.float32(-jnp.inf)

    def rcopy(src, dst, ss, rs, dev):
        return pltpu.make_async_remote_copy(src_ref=src, dst_ref=dst, send_sem=ss, recv_sem=rs,
                                            device_id={"ep": dev}, device_id_type=MESH)

    def w1_copy(i):
        s = i % ns1
        return pltpu.make_async_copy(
            w1.at[pl.ds((i % NG) * GE, GE), pl.ds((i // NG) * CW, CW), :], w1buf.at[s], w1sem.at[s])

    def w2_copy(i):
        s = i % ns2
        return pltpu.make_async_copy(
            w2.at[pl.ds((i % NG) * GE, GE), :, pl.ds((i // NG) * CW, CW)], w2buf.at[s], w2sem.at[s])

    def xown(c, core):
        return xr.at[c, pl.ds(core * TOK, TOK), :]

    def xlist(c, n, core):
        return xr.at[c, pl.ds(2 * TOK + (2 * n + core) * xb, xb), :]

    def x_copy(c):
        return pltpu.make_async_copy(tok.at[:, pl.ds(c * CW, CW)], xown(c, k), xsem.at[c])

    def p_copy(c, core):
        return rcopy(xown(c, core), xown(c, core), dsend.at[c * 7 + 6], drecv.at[c * DEV + 6], partner)

    def x_send(c, n):
        return rcopy(xs.at[c, pl.ds(n * xb, xb), :], xlist(c, n, k), dsend.at[c * 7 + n],
                     drecv.at[c * DEV + 2 * n + k], far[n])

    def x_fwd(c, n, core):
        return rcopy(xlist(c, n, core), xlist(c, n, core), dsend.at[c * 7 + 3 + n],
                     drecv.at[c * DEV + 2 * n + core], partner)

    barrier = pltpu.get_barrier_semaphore()
    for j in range(1, DEV):
        pl.semaphore_signal(barrier, inc=1, device_id={"ep": (me + j) % DEV}, device_id_type=MESH)
    log_copy = pltpu.make_async_copy(logit, log_s, nsem.at[0])
    log_copy.start()
    for c in range(NC):
        x_copy(c).start()
    log_copy.wait()

    def next_top(n, m):
        v = log_s[...]
        m = jnp.max(jnp.where(v < m, v, neg), axis=0, keepdims=True)
        cand[pl.ds(n, 1), :] = m
        return m

    lax.fori_loop(0, 8, next_top, jnp.full((1, ALL_EXP), jnp.inf, F32))
    pl.semaphore_wait(barrier, DEV - 1)

    def c_copy(j, src):
        return rcopy(cand, cands.at[pl.ds(src * 8, 8), :], csend.at[j], crecv.at[src], (me + j) % DEV)

    def k_copy(j, src):
        return rcopy(rk, rks.at[pl.ds(src * 8, 8), :], ksend.at[j], krecv.at[src], (me + j) % DEV)

    for j in range(1, DEV):
        c_copy(j, me).start()
    cands[pl.ds(me * 8, 8), :] = cand[...]

    def start_own(c, _):
        x_copy(c).wait()
        p_copy(c, k).start()
        return 0

    lax.fori_loop(0, NC, start_own, 0)
    if nx > 2 * TOK + 6 * xb:
        for c in range(NC):
            xr[c, 2 * TOK + 6 * xb:, :] = jnp.zeros((nx - 2 * TOK - 6 * xb, CW), BF16)
    t0, t1 = iota((TOK, TOK), 0), iota((TOK, TOK), 1)
    tri = onehot(t0 < t1)
    for j in range(1, DEV):
        c_copy(j, (me + j) % DEV).wait_recv()

    def next_max(_, m):
        v = cands[...]
        return jnp.max(jnp.where(v < m, v, neg), axis=0, keepdims=True)

    thr = lax.fori_loop(0, CAP, next_max, jnp.full((1, ALL_EXP), jnp.inf, F32))

    mo = onehot(log_s[...] >= thr)
    of_chip = onehot((iota((16, ALL_EXP), 1) >> 6) == iota((16, ALL_EXP), 0))
    used = dot_nt(of_chip, mo) > 0.5
    rt_s[...] = jnp.where(used, dot(onehot(used), tri), -1.0)
    xio = iota((xb, TOK), 0).astype(F32)
    for n in range(3):
        w_s[n * xb:(n + 1) * xb, :] = onehot(rt_s[pl.ds(far[n] // 2, 1), :] == xio)

    def compact(c, _):
        xs[c] = dot(w_s[...], xr[c, pl.ds(k * TOK, TOK), :]).astype(BF16)
        for n in (2, 0, 1):
            x_send(c, n).start()
        return 0

    compact(0, 0)

    of_chip2 = onehot((iota((ALL_EXP, 128), 0) >> 6) == iota((ALL_EXP, 128), 1))
    used2 = onehot(dot(mo, of_chip2) > 0.5)
    place = dot(onehot(t1 < t0), used2)
    place = jnp.where(iota((TOK, 128), 1) == chip, iota((TOK, 128), 0).astype(F32), place)
    place = dot_nt(place.astype(BF16), of_chip2)
    c64_s[...] = place

    def top_place(n, _):
        hit = log_s[...] == cand[pl.ds(n, 1), :]
        rk[pl.ds(n, 1), :] = jnp.max(jnp.where(hit, c64_s[...], -1.0), axis=0, keepdims=True)
        return 0

    lax.fori_loop(0, 8, top_place, 0)
    for j in range(1, DEV):
        k_copy(j, me).start()
    rks[pl.ds(me * 8, 8), :] = rk[...]
    lax.fori_loop(1, NC, compact, 0)
    for i in range(ns1):
        w1_copy(i).start()
    for i in range(ns2):
        w2_copy(i).start()

    cv = cands[...]
    sel = cv >= thr
    so = onehot(sel)
    j0, j1 = iota((64, 64), 0), iota((64, 64), 1)
    slot = dot(onehot(j1 < j0), so)
    inside = dot(onehot((j1 < j0) & ((j1 >> 4) == (j0 >> 4))), so)
    num = dot(onehot((j1 >> 4) == (j0 >> 4)), so)
    base = dot(num.astype(BF16), onehot((t0 < t1) & ((t0 >> 5) == (t1 >> 5))))
    rank = base + inside
    over = jnp.max(jnp.max(base + num, axis=0, keepdims=True), axis=1, keepdims=True) > bound
    c64_s[:64, :] = jnp.where(sel, rank, -1.0)

    pair = jnp.full((TOK, ALL_EXP), -1.0, F32)
    for n in range(8):
        pair = jnp.where(log_s[...] == cand[n:n + 1, :], c64_s[pl.ds(me * 8 + n, 1), :], pair)
    r2_s[...] = pair.T
    la = log_s[...].T
    ex = jnp.exp(la - jnp.max(la, axis=0, keepdims=True))
    gt_s[...] = ex / jnp.sum(ex, axis=0, keepdims=True)

    for j in range(1, DEV):
        k_copy(j, (me + j) % DEV).wait_recv()
    rv = rks[...]
    src = iota((64, ALL_EXP), 0) >> 3
    exp_chip = iota((64, ALL_EXP), 1) >> 6
    wide = jnp.max(jnp.max(jnp.where(sel & ((src >> 1) != exp_chip), rv, -1.0), axis=0, keepdims=True),
                   axis=1, keepdims=True) >= xb
    flag_out[0, 0] = jnp.max(jnp.where(over | wide, 1.0, 0.0)).astype(jnp.int32)
    rel = (src >> 1) ^ chip
    start = jnp.where(rel == 0, (src & 1) * TOK, 2 * TOK + (2 * (rel - 1) + (src & 1)) * xb).astype(F32)
    pos = start + rv + 1.0
    code = ((src >> 1) * 1024).astype(F32) + rank + 1.0
    pos_rows, code_rows = [], []
    for i in range(CAP):
        hit = sel & (slot == i)
        pos_rows.append(jnp.sum(jnp.where(hit, pos, 0.0), axis=0, keepdims=True))
        code_rows.append(jnp.sum(jnp.where(hit, code, 0.0), axis=0, keepdims=True))
    turn = ALL_EXP - me * EXP
    pos = pltpu.roll(jnp.concatenate(pos_rows, axis=0), turn, 1)
    code = pltpu.roll(jnp.concatenate(code_rows, axis=0), turn, 1)
    pio = iota((CAP, nx), 1).astype(F32) + 1.0
    for e in range(EXP):
        p_s[e * CAP:(e + 1) * CAP, :] = onehot(pos[:, e:e + 1] == pio)
        v_s[e * CAP:(e + 1) * CAP, :] = jnp.broadcast_to(code[:, e:e + 1], (CAP, 128))
    vt_s[...] = v_s[...].T[:8, :]
    rio = iota((bound, SLOTS), 0)
    for n, d in enumerate((xn, yn, dg, me)):
        want = (rio + ((d // 2) * 1024 + 1)).astype(F32)
        q_s[n * bound:(n + 1) * bound, :] = onehot(vt_s[0:1, :] == want)
    hacc[...] = jnp.zeros((SLOTS, FF), F32)

    def x_forward(c):
        for n in range(3):
            x_fwd(c, n, k).wait_recv()
            x_fwd(c, n, k).start()

    def first_product(c, last):
        for n in range(3):
            x_fwd(c, n, 1 - k).wait_recv()
        p_copy(c, 1 - k).wait_recv()
        pick_s[...] = dot(p_s[...], xr[c]).astype(BF16)

        def group(g, _):
            i = c * NG + 2 * g
            w1_copy(i).wait()
            w1_copy(i + 1).wait()
            for j in range(2 * GE):
                rows = pl.ds(g * (2 * GE * CAP) + j * CAP, CAP)
                v = hacc[rows, :] + dot(pick_s[rows, :], w1buf[(i + j // GE) % ns1, j % GE])
                if last:
                    h_s[rows, :] = gelu(v).astype(BF16)
                else:
                    hacc[rows, :] = v

            for n in (i, i + 1):
                @pl.when(n + ns1 < ITEMS)
                def _():
                    w1_copy(n + ns1).start()

            return 0

        lax.fori_loop(0, NG // 2, group, 0)

    def chunk(c, _):
        x_forward(c + 1)
        first_product(c, False)
        return 0

    x_forward(0)
    lax.fori_loop(0, NC - 1, chunk, 0)
    first_product(NC - 1, True)

    def rblk(c, d):
        return recv.at[c, pl.ds(d * bound, bound), :]

    def z_copy(c, n, dev):
        src = rblk(c, me) if n == 3 else zs.at[c, pl.ds(n * bound, bound), :]
        return rcopy(src, rblk(c, me), rsend.at[c * 7 + n], rrecv.at[c * DEV + me], dev)

    def fwd_copy(c, n, block):
        return rcopy(rblk(c, block), rblk(c, block), rsend.at[c * 7 + 4 + n], rrecv.at[c * DEV + block], partner)

    def second_product(c, _):
        def group(g, _):
            i = c * NG + 2 * g
            w2_copy(i).wait()
            w2_copy(i + 1).wait()
            for j in range(2 * GE):
                rows = pl.ds(g * (2 * GE * CAP) + j * CAP, CAP)
                zc_s[rows, :] = dot(h_s[rows, :], w2buf[(i + j // GE) % ns2, j % GE]).astype(BF16)

            for n in (i, i + 1):
                @pl.when(n + ns2 < ITEMS)
                def _():
                    w2_copy(n + ns2).start()

            return 0

        lax.fori_loop(0, NG // 2, group, 0)
        zc = zc_s[...]
        zs[c] = dot(q_s[:3 * bound, :], zc).astype(BF16)
        recv[c, pl.ds(me * bound, bound), :] = dot(q_s[3 * bound:, :], zc).astype(BF16)
        for n, dev in ((2, dg), (0, xn), (1, yn), (3, partner)):
            z_copy(c, n, dev).start()
        return 0

    lax.fori_loop(0, NC, second_product, 0)

    RB = 64

    def build_a(n, _):
        o = n // (bound // RB)
        r0 = (n % (bound // RB)) * RB
        rio2 = (iota((RB, TOK), 0) + r0).astype(F32)

        def one(e, acc):
            row = pl.ds(o * EXP + e, 1)
            return jnp.where(r2_s[row, :] == rio2, gt_s[row, :], acc)

        at_s[pl.ds(o * bound + r0, RB), :] = lax.fori_loop(0, EXP, one, jnp.zeros((RB, TOK), F32), unroll=8)
        return 0

    lax.fori_loop(0, DEV * (bound // RB), build_a, 0)

    def split_a(j, _):
        a = at_s[pl.ds(j * 128, 128), :].T
        for n in range(3):
            part = a.astype(BF16)
            a_s[n, :, pl.ds(j * 128, 128)] = part
            a = a - part.astype(F32)
        return 0

    lax.fori_loop(0, DEV * bound // 128, split_a, 0)

    def forward(c):
        for n, d in enumerate((xn, yn, dg)):
            fwd_copy(c, n, d).wait_recv()
            fwd_copy(c, n, d).start()

    def out_copy(c):
        return pltpu.make_async_copy(out_s.at[c], out.at[:, pl.ds(c * CW, CW)], osem.at[c])

    def combine(c):
        for d in (partner, xn + other, yn + other, dg + other):
            fwd_copy(c, 0, d).wait_recv()
        z = recv[c]
        y = dot(a_s[2], z) + dot(a_s[1], z) + dot(a_s[0], z)
        out_s[c] = (xr[c, pl.ds(k * TOK, TOK), :].astype(F32) + y).astype(BF16)
        out_copy(c).start()

    for j in range(1, DEV):
        c_copy(j, me).wait_send()
        k_copy(j, me).wait_send()

    def drain_x(c, _):
        p_copy(c, k).wait_send()
        for n in range(3):
            x_send(c, n).wait_send()
            x_fwd(c, n, k).wait_send()
        return 0

    lax.fori_loop(0, NC, drain_x, 0)

    def drain_z(c):
        for n, dev in enumerate((xn, yn, dg, partner)):
            z_copy(c, n, dev).wait_send()
        for n, d in enumerate((xn, yn, dg)):
            fwd_copy(c, n, d).wait_send()
        out_copy(c).wait()

    forward(0)

    def step(c, _):
        forward(c + 1)
        combine(c)

        @pl.when(c > 0)
        def _():
            drain_z(c - 1)

        return 0

    lax.fori_loop(0, NC - 1, step, 0)
    combine(NC - 1)
    drain_z(NC - 2)
    drain_z(NC - 1)


def moe_call(xb, bound, ns1, ns2, cid, tok, logit, w1, w2):
    nx = -(-(2 * TOK + 6 * xb) // 128) * 128
    vm = pltpu.VMEM
    sem = pltpu.SemaphoreType.DMA
    sq = vm((ALL_EXP, TOK), F32)
    return pl.pallas_call(
        functools.partial(moe_kernel, xb, nx, bound, ns1, ns2),
        out_shape=(jax.ShapeDtypeStruct((TOK, D), BF16), jax.ShapeDtypeStruct((1, 1), jnp.int32)),
        in_specs=[pl.BlockSpec(memory_space=pl.ANY)] * 4,
        out_specs=(pl.BlockSpec(memory_space=pl.ANY), pl.BlockSpec(memory_space=pltpu.SMEM)),
        scratch_shapes=[
            vm((NC, nx, CW), BF16), vm((NC, 3 * xb, CW), BF16),
            vm((ns1, GE, CW, FF), BF16), vm((ns2, GE, FF, CW), BF16),
            sq, vm((8, ALL_EXP), F32), vm((64, ALL_EXP), F32), vm((8, ALL_EXP), F32), vm((64, ALL_EXP), F32),
            vm((16, TOK), F32), vm((3 * xb, TOK), BF16), sq,
            vm((SLOTS, nx), BF16), vm((SLOTS, 128), F32), vm((8, SLOTS), F32), vm((4 * bound, SLOTS), BF16),
            vm((SLOTS, CW), BF16), vm((SLOTS, FF), F32), vm((SLOTS, FF), BF16), vm((SLOTS, CW), BF16),
            vm((NC, 3 * bound, CW), BF16), vm((NC, DEV * bound, CW), BF16),
            sq, sq, vm((DEV * bound, TOK), F32), vm((3, TOK, DEV * bound), BF16), vm((NC, TOK, CW), BF16),
            sem((ns1,)), sem((ns2,)), sem((NC,)), sem((NC,)), sem((DEV,)), sem((DEV,)), sem((DEV,)), sem((DEV,)),
            sem((1,)), sem((NC * 7,)), sem((NC * DEV,)), sem((NC * 7,)), sem((NC * DEV,)),
        ],
        compiler_params=pltpu.CompilerParams(collective_id=cid, has_side_effects=True, vmem_limit_bytes=67043328),
        name=f"moe_{bound}",
    )(tok, logit, w1, w2)


def solution(mesh):
    row_spec = P(("dp", "ep"), None)
    expert_spec = P("ep", None, None)

    def device_step(tok, logit, w1, w2):
        out, flag = moe_call(144, 192, 8, 8, 0, tok, logit, w1, w2)
        return lax.switch(flag[0, 0], (lambda: out, lambda: moe_call(TOK, 512, 2, 2, 1, tok, logit, w1, w2)[0]))

    return jax.shard_map(device_step, mesh=mesh, in_specs=(row_spec, row_spec, expert_spec, expert_spec),
                         out_specs=row_spec, check_vma=False)
```

```python
import functools

import jax
import jax.numpy as jnp
from jax import lax
from jax.experimental import pallas as pl
from jax.experimental.pallas import tpu as pltpu
from jax.sharding import PartitionSpec as P

MESH = pl.DeviceIdType.MESH
F32, BF16 = jnp.float32, jnp.bfloat16
DEV = 8
TOK = 256
D = 2048
FF = 512
EXP = 32
ALL_EXP = EXP * DEV
CAP = 16
SLOTS = EXP * CAP
NC = 8
CW = D // NC
GE = 8
NG = EXP // GE
ITEMS = NC * NG


def dot(a, b):
    return jnp.dot(a, b, preferred_element_type=F32)


def iota(shape, dim):
    return lax.broadcasted_iota(jnp.int32, shape, dim)


def gelu(v):
    return 0.5 * v * (1.0 + lax.erf(v * 0.7071067811865476))


def dot_nt(a, b):
    return lax.dot_general(a, b, (((1,), (1,)), ((), ())), preferred_element_type=F32)


def onehot(cond):
    return jnp.where(cond, 1.0, 0.0).astype(BF16)


def moe_kernel(xb, nx, bound, ns1, ns2, tok, logit, w1, w2, out, flag_out,
               xr, xs, w1buf, w2buf, log_s, cand, cands, rk, rks, rt_s, w_s, c64_s,
               p_s, v_s, vt_s, q_s, pick_s, hacc, h_s, zc_s, zs, recv,
               r2_s, gt_s, at_s, a_s, out_s,
               w1sem, w2sem, xsem, osem, lsem, csend, crecv, ksend, krecv, xsend, xfsend, psend, precv, xrecv, xfrecv,
               zsend, zfsend, osend, zrecv, zfrecv):
    split = ns1 >= NG and ns2 >= NG
    me = lax.axis_index("ep")
    k = me % 2
    chip = me // 2
    cx = chip % 2
    cy = chip // 2
    dx = 2 - 4 * cx
    dy = 4 - 8 * cy
    other = 1 - 2 * k
    partner = me + other
    xn, yn, dg = me + dx, me + dy, me + dx + dy
    far = (xn, yn, dg)
    neg = jnp.float32(-jnp.inf)

    def rcopy(src, dst, ss, rs, dev):
        return pltpu.make_async_remote_copy(src_ref=src, dst_ref=dst, send_sem=ss, recv_sem=rs,
                                            device_id={"ep": dev}, device_id_type=MESH)

    def w1_copy(i):
        s = i % ns1
        return pltpu.make_async_copy(
            w1.at[pl.ds((i % NG) * GE, GE), pl.ds((i // NG) * CW, CW), :], w1buf.at[s], w1sem.at[s])

    def w2_copy(i):
        s = i % ns2
        return pltpu.make_async_copy(
            w2.at[pl.ds((i % NG) * GE, GE), :, pl.ds((i // NG) * CW, CW)], w2buf.at[s], w2sem.at[s])

    def xown(c, core):
        return xr.at[c, pl.ds(core * TOK, TOK), :]

    def xlist(c, n, core):
        return xr.at[c, pl.ds(2 * TOK + (2 * n + core) * xb, xb), :]

    def x_copy(c):
        return pltpu.make_async_copy(tok.at[:, pl.ds(c * CW, CW)], xown(c, k), xsem)

    def await_bytes(ref, sem):
        pltpu.make_async_copy(ref, ref, sem).wait()

    def lanes(h):
        return pl.ds(0, CW) if h is None else pl.ds(h * (CW // 2), CW // 2)

    def p_copy(c):
        return rcopy(xown(c, k), xown(c, k), psend, precv, partner)

    def x_unit(c, h):
        return NC if h == 1 else c

    def x_send(c, n, h=None):
        return rcopy(xs.at[c, pl.ds(n * xb, xb), lanes(h)], xlist(c, n, k).at[:, lanes(h)], xsend,
                     xrecv.at[x_unit(c, h)], far[n])

    def x_fwd(c, n, h=None):
        block = xlist(c, n, k).at[:, lanes(h)]
        return rcopy(block, block, xfsend, xfrecv.at[x_unit(c, h)], partner)

    barrier = pltpu.get_barrier_semaphore()
    for j in range(1, DEV):
        pl.semaphore_signal(barrier, inc=1, device_id={"ep": (me + j) % DEV}, device_id_type=MESH)
    log_copy = pltpu.make_async_copy(logit, log_s, lsem)
    log_copy.start()
    for c in range(NC):
        x_copy(c).start()
    log_copy.wait()

    def next_top(n, m):
        v = log_s[...]
        m = jnp.max(jnp.where(v < m, v, neg), axis=0, keepdims=True)
        cand[pl.ds(n, 1), :] = m
        return m

    lax.fori_loop(0, 8, next_top, jnp.full((1, ALL_EXP), jnp.inf, F32))
    pl.semaphore_wait(barrier, DEV - 1)

    def c_copy(j):
        return rcopy(cand, cands.at[pl.ds(me * 8, 8), :], csend, crecv, (me + j) % DEV)

    def k_copy(j):
        return rcopy(rk, rks.at[pl.ds(me * 8, 8), :], ksend, krecv, (me + j) % DEV)

    seven = cands.at[pl.ds(0, 8 * (DEV - 1)), :]
    for j in range(1, DEV):
        c_copy(j).start()
    cands[pl.ds(me * 8, 8), :] = cand[...]

    await_bytes(out_s, xsem)
    for c in range(NC):
        p_copy(c).start()
    if nx > 2 * TOK + 6 * xb:
        for c in range(NC):
            xr[c, 2 * TOK + 6 * xb:, :] = jnp.zeros((nx - 2 * TOK - 6 * xb, CW), BF16)
    t0, t1 = iota((TOK, TOK), 0), iota((TOK, TOK), 1)
    tri = onehot(t0 < t1)
    await_bytes(seven, crecv)

    def next_max(_, m):
        v = cands[...]
        return jnp.max(jnp.where(v < m, v, neg), axis=0, keepdims=True)

    thr = lax.fori_loop(0, CAP, next_max, jnp.full((1, ALL_EXP), jnp.inf, F32))

    mo = onehot(log_s[...] >= thr)
    of_chip = onehot((iota((16, ALL_EXP), 1) >> 6) == iota((16, ALL_EXP), 0))
    used = dot_nt(of_chip, mo) > 0.5
    rt_s[...] = jnp.where(used, dot(onehot(used), tri), -1.0)
    xio = iota((xb, TOK), 0).astype(F32)
    for n in range(3):
        w_s[n * xb:(n + 1) * xb, :] = onehot(rt_s[pl.ds(far[n] // 2, 1), :] == xio)

    def compact(c, _):
        xs[c] = dot(w_s[...], xr[c, pl.ds(k * TOK, TOK), :]).astype(BF16)
        for n in (2, 0, 1):
            x_send(c, n).start()
        return 0

    compact(0, 0)

    of_chip2 = onehot((iota((ALL_EXP, 128), 0) >> 6) == iota((ALL_EXP, 128), 1))
    used2 = onehot(dot(mo, of_chip2) > 0.5)
    place = dot(onehot(t1 < t0), used2)
    place = jnp.where(iota((TOK, 128), 1) == chip, iota((TOK, 128), 0).astype(F32), place)
    place = dot_nt(place.astype(BF16), of_chip2)
    c64_s[...] = place

    def top_place(n, _):
        hit = log_s[...] == cand[pl.ds(n, 1), :]
        rk[pl.ds(n, 1), :] = jnp.max(jnp.where(hit, c64_s[...], -1.0), axis=0, keepdims=True)
        return 0

    lax.fori_loop(0, 8, top_place, 0)
    for j in range(1, DEV):
        k_copy(j).start()
    rks[pl.ds(me * 8, 8), :] = rk[...]
    lax.fori_loop(1, NC - 1, compact, 0)
    if split:
        xs[NC - 1] = dot(w_s[...], xr[NC - 1, pl.ds(k * TOK, TOK), :]).astype(BF16)
        for h in range(2):
            for n in (2, 0, 1):
                x_send(NC - 1, n, h).start()
    else:
        compact(NC - 1, 0)
    for i in range(ns1):
        w1_copy(i).start()
    for i in range(ns2):
        w2_copy(i).start()

    cv = cands[...]
    sel = cv >= thr
    so = onehot(sel)
    j0, j1 = iota((64, 64), 0), iota((64, 64), 1)
    slot = dot(onehot(j1 < j0), so)
    inside = dot(onehot((j1 < j0) & ((j1 >> 4) == (j0 >> 4))), so)
    num = dot(onehot((j1 >> 4) == (j0 >> 4)), so)
    base = dot(num.astype(BF16), onehot((t0 < t1) & ((t0 >> 5) == (t1 >> 5))))
    rank = base + inside
    over = jnp.max(jnp.max(base + num, axis=0, keepdims=True), axis=1, keepdims=True) > bound
    c64_s[:64, :] = jnp.where(sel, rank, -1.0)

    pair = jnp.full((TOK, ALL_EXP), -1.0, F32)
    for n in range(8):
        pair = jnp.where(log_s[...] == cand[n:n + 1, :], c64_s[pl.ds(me * 8 + n, 1), :], pair)
    r2_s[...] = pair.T
    la = log_s[...].T
    ex = jnp.exp(la - jnp.max(la, axis=0, keepdims=True))
    gt_s[...] = ex / jnp.sum(ex, axis=0, keepdims=True)

    await_bytes(seven, krecv)
    rv = rks[...]
    src = iota((64, ALL_EXP), 0) >> 3
    exp_chip = iota((64, ALL_EXP), 1) >> 6
    wide = jnp.max(jnp.max(jnp.where(sel & ((src >> 1) != exp_chip), rv, -1.0), axis=0, keepdims=True),
                   axis=1, keepdims=True) >= xb
    flag_out[0, 0] = jnp.max(jnp.where(over | wide, 1.0, 0.0)).astype(jnp.int32)
    rel = (src >> 1) ^ chip
    start = jnp.where(rel == 0, (src & 1) * TOK, 2 * TOK + (2 * (rel - 1) + (src & 1)) * xb).astype(F32)
    pos = start + rv + 1.0
    code = ((src >> 1) * 1024).astype(F32) + rank + 1.0
    pos_rows, code_rows = [], []
    for i in range(CAP):
        hit = sel & (slot == i)
        pos_rows.append(jnp.sum(jnp.where(hit, pos, 0.0), axis=0, keepdims=True))
        code_rows.append(jnp.sum(jnp.where(hit, code, 0.0), axis=0, keepdims=True))
    turn = ALL_EXP - me * EXP
    pos = pltpu.roll(jnp.concatenate(pos_rows, axis=0), turn, 1)
    code = pltpu.roll(jnp.concatenate(code_rows, axis=0), turn, 1)
    pio = iota((CAP, nx), 1).astype(F32) + 1.0
    for e in range(EXP):
        p_s[e * CAP:(e + 1) * CAP, :] = onehot(pos[:, e:e + 1] == pio)
        v_s[e * CAP:(e + 1) * CAP, :] = jnp.broadcast_to(code[:, e:e + 1], (CAP, 128))
    vt_s[...] = v_s[...].T[:8, :]
    rio = iota((bound, SLOTS), 0)
    for n, d in enumerate((xn, yn, dg, me)):
        want = (rio + ((d // 2) * 1024 + 1)).astype(F32)
        q_s[n * bound:(n + 1) * bound, :] = onehot(vt_s[0:1, :] == want)
    hacc[...] = jnp.zeros((SLOTS, FF), F32)

    def x_forward(c, h=None):
        await_bytes(xs.at[c, :, lanes(h)], xrecv.at[x_unit(c, h)])
        for n in range(3):
            x_fwd(c, n, h).start()

    def first_product(c, last, h=None):
        cols = lanes(h)
        await_bytes(xs.at[c, :, cols], xfrecv.at[x_unit(c, h)])
        pick_s[:, cols] = dot(p_s[...], xr[c, :, cols]).astype(BF16)

        def group(g, _):
            i = c * NG + 2 * g
            if h != 1:
                w1_copy(i).wait()
                w1_copy(i + 1).wait()
            for j in range(2 * GE):
                rows = pl.ds(g * (2 * GE * CAP) + j * CAP, CAP)
                v = hacc[rows, :] + dot(pick_s[rows, cols], w1buf[(i + j // GE) % ns1, j % GE, cols, :])
                if last:
                    h_s[rows, :] = gelu(v).astype(BF16)
                else:
                    hacc[rows, :] = v

            if h is None:
                for n in (i, i + 1):
                    @pl.when(n + ns1 < ITEMS)
                    def _():
                        w1_copy(n + ns1).start()

            return 0

        lax.fori_loop(0, NG // 2, group, 0)

    def chunk(c, _):
        x_forward(c + 1)
        first_product(c, False)
        return 0

    await_bytes(out_s, precv)
    x_forward(0)
    lax.fori_loop(0, NC - 2, chunk, 0)
    if split:
        x_forward(NC - 1, 0)
        first_product(NC - 2, False)
        x_forward(NC - 1, 1)
        first_product(NC - 1, False, 0)
        first_product(NC - 1, True, 1)
    else:
        x_forward(NC - 1)
        first_product(NC - 2, False)
        first_product(NC - 1, True)

    def rblk(c, d, h):
        return recv.at[c, pl.ds(d * bound, bound), lanes(h)]

    def z_unit(c, h):
        return c if h != 1 else (NC if c == 0 else NC + 1)

    def z_copy(c, n, dev, h=None):
        block = rblk(c, me, h)
        if n == 3:
            return rcopy(block, block, osend, zfrecv.at[c if h is None or c == 0 else z_unit(c, h)], dev)
        return rcopy(zs.at[c, pl.ds(n * bound, bound), lanes(h)], block, zsend, zrecv.at[z_unit(c, h)], dev)

    def fwd_copy(c, d, h=None):
        return rcopy(rblk(c, d, h), rblk(c, d, h), zfsend, zfrecv.at[z_unit(c, h)], partner)

    def second_product(c, h=None):
        cols = lanes(h)

        def group(g, _):
            i = c * NG + 2 * g
            if h != 1:
                w2_copy(i).wait()
                w2_copy(i + 1).wait()
            for j in range(2 * GE):
                rows = pl.ds(g * (2 * GE * CAP) + j * CAP, CAP)
                zc_s[rows, cols] = dot(h_s[rows, :], w2buf[(i + j // GE) % ns2, j % GE, :, cols]).astype(BF16)

            if h != 0:
                for n in (i, i + 1):
                    @pl.when(n + ns2 < ITEMS)
                    def _():
                        w2_copy(n + ns2).start()

            return 0

        lax.fori_loop(0, NG // 2, group, 0)
        zc = zc_s[:, cols]
        zs[c, :, cols] = dot(q_s[:3 * bound, :], zc).astype(BF16)
        recv[c, pl.ds(me * bound, bound), cols] = dot(q_s[3 * bound:, :], zc).astype(BF16)
        for n, dev in ((2, dg), (0, xn), (1, yn), (3, partner)):
            z_copy(c, n, dev, h).start()

    def second(c, _):
        second_product(c)
        return 0

    if split:
        second_product(0, 0)
        second_product(0, 1)
        lax.fori_loop(1, NC - 1, second, 0)
        second_product(NC - 1, 0)
        second_product(NC - 1, 1)
    else:
        lax.fori_loop(0, NC, second, 0)

    RB = 64

    def build_a(n, _):
        o = n // (bound // RB)
        r0 = (n % (bound // RB)) * RB
        rio2 = (iota((RB, TOK), 0) + r0).astype(F32)

        def one(e, acc):
            row = pl.ds(o * EXP + e, 1)
            return jnp.where(r2_s[row, :] == rio2, gt_s[row, :], acc)

        at_s[pl.ds(o * bound + r0, RB), :] = lax.fori_loop(0, EXP, one, jnp.zeros((RB, TOK), F32), unroll=8)
        return 0

    lax.fori_loop(0, DEV * (bound // RB), build_a, 0)

    def split_a(j, _):
        a = at_s[pl.ds(j * 128, 128), :].T
        for n in range(3):
            part = a.astype(BF16)
            a_s[n, :, pl.ds(j * 128, 128)] = part
            a = a - part.astype(F32)
        return 0

    lax.fori_loop(0, DEV * bound // 128, split_a, 0)

    def forward(c, h=None):
        if split and h is None and isinstance(c, int):
            await_bytes(zs.at[c, :, lanes(0)], zrecv.at[z_unit(c, 0)])
            await_bytes(zs.at[c, :, lanes(1)], zrecv.at[z_unit(c, 1)])
        else:
            await_bytes(zs.at[c, :, lanes(h)], zrecv.at[z_unit(c, h)])
        for d in far:
            fwd_copy(c, d, h).start()

    def out_copy(c, h):
        half = 0 if h is None else h * (CW // 2)
        return pltpu.make_async_copy(out_s.at[c, :, lanes(h)],
                                     out.at[:, pl.ds(c * CW + half, CW if h is None else CW // 2)], osem)

    def combine(c, h=None):
        cols = lanes(h)
        await_bytes(recv.at[c, pl.ds(0, 4 * bound), cols], zfrecv.at[z_unit(c, h)])
        z = recv[c, :, cols]
        y = dot(a_s[2], z) + dot(a_s[1], z) + dot(a_s[0], z)
        out_s[c, :, cols] = (xr[c, pl.ds(k * TOK, TOK), cols].astype(F32) + y).astype(BF16)
        out_copy(c, h).start()

    def step(c, _):
        forward(c + 1)
        combine(c)
        return 0

    await_bytes(seven, csend)
    await_bytes(seven, ksend)
    await_bytes(out_s, psend)
    await_bytes(xs, xsend)
    await_bytes(xs, xfsend)
    forward(0)
    lax.fori_loop(0, NC - 2, step, 0)
    if split:
        forward(NC - 1, 0)
        combine(NC - 2)
        forward(NC - 1, 1)
        combine(NC - 1, 0)
        combine(NC - 1, 1)
    else:
        forward(NC - 1)
        combine(NC - 2)
        combine(NC - 1)
    await_bytes(zs, zsend)
    await_bytes(recv.at[:, pl.ds(0, bound), :], osend)
    await_bytes(zs, zfsend)
    await_bytes(out_s, osem)


def moe_call(xb, bound, ns1, ns2, cid, tok, logit, w1, w2):
    nx = -(-(2 * TOK + 6 * xb) // 128) * 128
    vm = pltpu.VMEM
    sem = pltpu.SemaphoreType.DMA
    sq = vm((ALL_EXP, TOK), F32)
    return pl.pallas_call(
        functools.partial(moe_kernel, xb, nx, bound, ns1, ns2),
        out_shape=(jax.ShapeDtypeStruct((TOK, D), BF16), jax.ShapeDtypeStruct((1, 1), jnp.int32)),
        in_specs=[pl.BlockSpec(memory_space=pl.ANY)] * 4,
        out_specs=(pl.BlockSpec(memory_space=pl.ANY), pl.BlockSpec(memory_space=pltpu.SMEM)),
        scratch_shapes=[
            vm((NC, nx, CW), BF16), vm((NC, 3 * xb, CW), BF16),
            vm((ns1, GE, CW, FF), BF16), vm((ns2, GE, FF, CW), BF16),
            sq, vm((8, ALL_EXP), F32), vm((64, ALL_EXP), F32), vm((8, ALL_EXP), F32), vm((64, ALL_EXP), F32),
            vm((16, TOK), F32), vm((3 * xb, TOK), BF16), sq,
            vm((SLOTS, nx), BF16), vm((SLOTS, 128), F32), vm((8, SLOTS), F32), vm((4 * bound, SLOTS), BF16),
            vm((SLOTS, CW), BF16), vm((SLOTS, FF), F32), vm((SLOTS, FF), BF16), vm((SLOTS, CW), BF16),
            vm((NC, 3 * bound, CW), BF16), vm((NC, DEV * bound, CW), BF16),
            sq, sq, vm((DEV * bound, TOK), F32), vm((3, TOK, DEV * bound), BF16), vm((NC, TOK, CW), BF16),
            sem((ns1,)), sem((ns2,)), *[sem] * 11, sem((NC + 1,)), sem((NC + 1,)), *[sem] * 3,
            sem((NC + 2,)), sem((NC + 2,)),
        ],
        compiler_params=pltpu.CompilerParams(collective_id=cid, has_side_effects=True, vmem_limit_bytes=67043328),
        name=f"moe_{bound}",
    )(tok, logit, w1, w2)


def solution(mesh):
    row_spec = P(("dp", "ep"), None)
    expert_spec = P("ep", None, None)

    def device_step(tok, logit, w1, w2):
        out, flag = moe_call(144, 192, 8, 8, 0, tok, logit, w1, w2)
        return lax.switch(flag[0, 0], (lambda: out, lambda: moe_call(TOK, 512, 2, 2, 1, tok, logit, w1, w2)[0]))

    return jax.shard_map(device_step, mesh=mesh, in_specs=(row_spec, row_spec, expert_spec, expert_spec),
                         out_specs=row_spec, check_vma=False)
```

```python
import functools

import jax
import jax.numpy as jnp
from jax import lax
from jax.experimental import pallas as pl
from jax.experimental.pallas import tpu as pltpu
from jax.sharding import PartitionSpec as P

MESH = pl.DeviceIdType.MESH
F32, BF16 = jnp.float32, jnp.bfloat16
DEV = 8
TOK = 256
D = 2048
FF = 512
EXP = 32
ALL_EXP = EXP * DEV
CAP = 16
SLOTS = EXP * CAP
NC = 8
CW = D // NC
HW = CW // 2


def dot(a, b):
    return jnp.dot(a, b, preferred_element_type=F32)


def iota(shape, dim):
    return lax.broadcasted_iota(jnp.int32, shape, dim)


def gelu(v):
    return 0.5 * v * (1.0 + lax.erf(v * 0.7071067811865476))


def dot_nt(a, b):
    return lax.dot_general(a, b, (((1,), (1,)), ((), ())), preferred_element_type=F32)


def onehot(cond):
    return jnp.where(cond, 1.0, 0.0).astype(BF16)


def moe_kernel(xb, nx, bound, ge, ns1, ns2, nz, tok, logit, w1, w2, out, flag_out,
               xr, xs, w1buf, w2buf, log_s, cand, cands, rk, rks, rt_s, w_s, c64_s,
               p_s, v_s, vt_s, q_s, pick_s, hacc, h_s, zc_s, zq, zin, zown, zs, recv,
               r2_s, gt_s, at_s, a_s, out_s,
               w1sem, w2sem, xsem, osem, lsem, csend, crecv, ksend, krecv, xsend, xfsend, psend, precv, xrecv, xfrecv,
               zsend, zfsend, zrecv, zfrecv, qsend, qrecv):
    groups = EXP // ge
    items = NC * groups
    rows_in = recv.shape[1]
    me = lax.axis_index("ep")
    k = me % 2
    chip = me // 2
    cx = chip % 2
    cy = chip // 2
    dx = 2 - 4 * cx
    dy = 4 - 8 * cy
    other = 1 - 2 * k
    partner = me + other
    xn, yn, dg = me + dx, me + dy, me + dx + dy
    far = (xn, yn, dg)
    neg = jnp.float32(-jnp.inf)

    def rcopy(src, dst, ss, rs, dev):
        return pltpu.make_async_remote_copy(src_ref=src, dst_ref=dst, send_sem=ss, recv_sem=rs,
                                            device_id={"ep": dev}, device_id_type=MESH)

    def w1_copy(i):
        s = i % ns1
        return pltpu.make_async_copy(
            w1.at[pl.ds((i % groups) * ge, ge), pl.ds((i // groups) * CW, CW), :], w1buf.at[s], w1sem.at[s])

    def w2_copy(i):
        s = i % ns2
        return pltpu.make_async_copy(
            w2.at[pl.ds((i % groups) * ge, ge), :, pl.ds((i // groups) * CW, CW)], w2buf.at[s], w2sem.at[s])

    def xown(c, core):
        return xr.at[c, pl.ds(core * TOK, TOK), :]

    def xlist(c, n, core):
        return xr.at[c, pl.ds(2 * TOK + (2 * n + core) * xb, xb), :]

    def x_copy(c):
        return pltpu.make_async_copy(tok.at[:, pl.ds(c * CW, CW)], xown(c, k), xsem)

    def await_bytes(ref, sem):
        pltpu.make_async_copy(ref, ref, sem).wait()

    def p_copy(c):
        return rcopy(xown(c, k), xown(c, k), psend, precv, partner)

    def x_send(c, n):
        return rcopy(xs.at[c, pl.ds(n * xb, xb), :], xlist(c, n, k), xsend, xrecv.at[c], far[n])

    def x_fwd(c, n):
        return rcopy(xlist(c, n, k), xlist(c, n, k), xfsend, xfrecv.at[c], partner)

    log_copy = pltpu.make_async_copy(logit, log_s, lsem)
    log_copy.start()
    barrier = pltpu.get_barrier_semaphore()
    for j in range(1, DEV):
        pl.semaphore_signal(barrier, inc=1, device_id={"ep": (me + j) % DEV}, device_id_type=MESH)
    for c in range(NC):
        x_copy(c).start()
    log_copy.wait()

    def next_top(n, m):
        v = log_s[...]
        m = jnp.max(jnp.where(v < m, v, neg), axis=0, keepdims=True)
        cand[pl.ds(n, 1), :] = m
        return m

    lax.fori_loop(0, 8, next_top, jnp.full((1, ALL_EXP), jnp.inf, F32))
    pl.semaphore_wait(barrier, DEV - 1)

    def c_copy(j):
        return rcopy(cand, cands.at[pl.ds(me * 8, 8), :], csend, crecv, (me + j) % DEV)

    def k_copy(j):
        return rcopy(rk, rks.at[pl.ds(me * 8, 8), :], ksend, krecv, (me + j) % DEV)

    seven = cands.at[pl.ds(0, 8 * (DEV - 1)), :]
    for j in range(1, DEV):
        c_copy(j).start()
    cands[pl.ds(me * 8, 8), :] = cand[...]

    await_bytes(out_s, xsem)
    for c in range(NC):
        p_copy(c).start()
    if rows_in > 4 * bound:
        for c in range(NC):
            recv[c, 4 * bound:, :] = jnp.zeros((rows_in - 4 * bound, CW), BF16)
        at_s[4 * bound:, :] = jnp.zeros((rows_in - 4 * bound, TOK), F32)
    if nx > 2 * TOK + 6 * xb:
        for c in range(NC):
            xr[c, 2 * TOK + 6 * xb:, :] = jnp.zeros((nx - 2 * TOK - 6 * xb, CW), BF16)
    t0, t1 = iota((TOK, TOK), 0), iota((TOK, TOK), 1)
    tri = onehot(t0 < t1)
    await_bytes(seven, crecv)

    def next_max(_, m):
        v = cands[...]
        return jnp.max(jnp.where(v < m, v, neg), axis=0, keepdims=True)

    thr = lax.fori_loop(0, CAP, next_max, jnp.full((1, ALL_EXP), jnp.inf, F32))

    mo = onehot(log_s[...] >= thr)
    of_chip = onehot((iota((16, ALL_EXP), 1) >> 6) == iota((16, ALL_EXP), 0))
    used = dot_nt(of_chip, mo) > 0.5
    rt_s[...] = jnp.where(used, dot(onehot(used), tri), -1.0)
    xio = iota((xb, TOK), 0).astype(F32)
    for n in range(3):
        w_s[n * xb:(n + 1) * xb, :] = onehot(rt_s[pl.ds(far[n] // 2, 1), :] == xio)

    def compact(c, _):
        xs[c] = dot(w_s[...], xr[c, pl.ds(k * TOK, TOK), :]).astype(BF16)
        for n in (2, 0, 1):
            x_send(c, n).start()
        return 0

    compact(0, 0)

    of_chip2 = onehot((iota((ALL_EXP, 128), 0) >> 6) == iota((ALL_EXP, 128), 1))
    used2 = onehot(dot(mo, of_chip2) > 0.5)
    place = dot(onehot(t1 < t0), used2)
    place = jnp.where(iota((TOK, 128), 1) == chip, iota((TOK, 128), 0).astype(F32), place)
    place = dot_nt(place.astype(BF16), of_chip2)
    c64_s[...] = place

    def top_place(n, _):
        hit = log_s[...] == cand[pl.ds(n, 1), :]
        rk[pl.ds(n, 1), :] = jnp.max(jnp.where(hit, c64_s[...], -1.0), axis=0, keepdims=True)
        return 0

    lax.fori_loop(0, 8, top_place, 0)
    for j in range(1, DEV):
        k_copy(j).start()
    rks[pl.ds(me * 8, 8), :] = rk[...]
    lax.fori_loop(1, NC, compact, 0)
    for i in range(ns1):
        w1_copy(i).start()
    for i in range(ns2):
        w2_copy(i).start()

    cv = cands[...]
    sel = cv >= thr
    so = onehot(sel)
    j0, j1 = iota((64, 64), 0), iota((64, 64), 1)
    slot = dot(onehot(j1 < j0), so)
    inside = dot(onehot((j1 < j0) & ((j1 >> 4) == (j0 >> 4))), so)
    num = dot(onehot((j1 >> 4) == (j0 >> 4)), so)
    base = dot(num.astype(BF16), onehot((t0 < t1) & ((t0 >> 6) == (t1 >> 6))))
    rank = base + inside
    over = jnp.max(jnp.max(base + num, axis=0, keepdims=True), axis=1, keepdims=True) > bound
    c64_s[:64, :] = jnp.where(sel, rank, -1.0)

    pair = jnp.full((TOK, ALL_EXP), -1.0, F32)
    for n in range(8):
        pair = jnp.where(log_s[...] == cand[n:n + 1, :], c64_s[pl.ds(me * 8 + n, 1), :], pair)
    r2_s[...] = pair.T
    la = log_s[...].T
    ex = jnp.exp(la - jnp.max(la, axis=0, keepdims=True))
    gt_s[...] = ex / jnp.sum(ex, axis=0, keepdims=True)

    await_bytes(seven, krecv)
    rv = rks[...]
    src = iota((64, ALL_EXP), 0) >> 3
    exp_chip = iota((64, ALL_EXP), 1) >> 6
    wide = jnp.max(jnp.max(jnp.where(sel & ((src >> 1) != exp_chip), rv, -1.0), axis=0, keepdims=True),
                   axis=1, keepdims=True) >= xb
    flag_out[0, 0] = jnp.max(jnp.where(over | wide, 1.0, 0.0)).astype(jnp.int32)
    rel = (src >> 1) ^ chip
    start = jnp.where(rel == 0, (src & 1) * TOK, 2 * TOK + (2 * (rel - 1) + (src & 1)) * xb).astype(F32)
    pos = start + rv + 1.0
    code = ((src >> 1) * 1024).astype(F32) + rank + 1.0
    pos_rows, code_rows = [], []
    for i in range(CAP):
        hit = sel & (slot == i)
        pos_rows.append(jnp.sum(jnp.where(hit, pos, 0.0), axis=0, keepdims=True))
        code_rows.append(jnp.sum(jnp.where(hit, code, 0.0), axis=0, keepdims=True))
    turn = ALL_EXP - me * EXP
    pos = pltpu.roll(jnp.concatenate(pos_rows, axis=0), turn, 1)
    code = pltpu.roll(jnp.concatenate(code_rows, axis=0), turn, 1)
    pio = iota((CAP, nx), 1).astype(F32) + 1.0
    for e in range(EXP):
        p_s[e * CAP:(e + 1) * CAP, :] = onehot(pos[:, e:e + 1] == pio)
        v_s[e * CAP:(e + 1) * CAP, :] = jnp.broadcast_to(code[:, e:e + 1], (CAP, 128))
    vt_s[...] = v_s[...].T[:8, :]
    rio = iota((bound, SLOTS), 0)
    for n, d in enumerate((xn, yn, dg, me)):
        want = (rio + ((d // 2) * 1024 + 1)).astype(F32)
        q_s[n * bound:(n + 1) * bound, :] = onehot(vt_s[0:1, :] == want)
    hacc[...] = jnp.zeros((SLOTS, FF), F32)

    def x_forward(c):
        await_bytes(xs.at[c], xrecv.at[c])
        for n in range(3):
            x_fwd(c, n).start()

    def first_product(c, last):
        await_bytes(xs.at[c], xfrecv.at[c])
        pick_s[...] = dot(p_s[...], xr[c]).astype(BF16)

        def group(g, _):
            i = c * groups + 2 * g
            w1_copy(i).wait()
            w1_copy(i + 1).wait()
            for j in range(2 * ge):
                rows = pl.ds(g * (2 * ge * CAP) + j * CAP, CAP)
                v = hacc[rows, :] + dot(pick_s[rows, :], w1buf[(i + j // ge) % ns1, j % ge])
                if last:
                    h_s[rows, :] = gelu(v).astype(BF16)
                else:
                    hacc[rows, :] = v

            for n in (i, i + 1):
                @pl.when(n + ns1 < items)
                def _():
                    w1_copy(n + ns1).start()

            return 0

        lax.fori_loop(0, groups // 2, group, 0)

    def chunk(c, _):
        x_forward(c + 1)
        first_product(c, False)
        return 0

    await_bytes(out_s, precv)
    x_forward(0)
    lax.fori_loop(0, NC - 1, chunk, 0)
    first_product(NC - 1, True)

    RB = 64 if bound % 64 == 0 else 48

    def build_a(n, _):
        o = n // (bound // RB)
        r0 = (n % (bound // RB)) * RB
        rio2 = (iota((RB, TOK), 0) + r0).astype(F32)

        def one(e, acc):
            row = pl.ds(o * 2 * EXP + e, 1)
            return jnp.where(r2_s[row, :] == rio2, gt_s[row, :], acc)

        at_s[pl.ds(o * bound + r0, RB), :] = lax.fori_loop(0, 2 * EXP, one, jnp.zeros((RB, TOK), F32), unroll=8)
        return 0

    blocks = 4 * (bound // RB)
    turns = NC - 1 if blocks % (NC - 1) == 0 else NC
    per = blocks // turns

    mine = pl.ds(pl.multiple_of(k * HW, HW), HW)
    theirs = pl.ds(pl.multiple_of((1 - k) * HW, HW), HW)

    def rblk(c, d):
        return recv.at[c, pl.ds((d // 2) * bound, bound), mine]

    def q_copies(s):
        return (rcopy(zq.at[s, pl.ds(0, 3 * bound), theirs], zin.at[s], qsend.at[s], qrecv.at[s], partner),
                rcopy(zq.at[s, pl.ds(3 * bound, bound), :], zown.at[s], qsend.at[s], qrecv.at[s], partner))

    def z_copy(c, n, dev):
        return rcopy(zs.at[c % nz, pl.ds(n * bound, bound), :], rblk(c, me), zsend.at[c % nz], zrecv.at[c], dev)

    def fwd_copy(c, d):
        return rcopy(rblk(c, d), rblk(c, d), zfsend, zfrecv.at[c], partner)

    def q_bytes(s):
        return zq.at[s, pl.ds(0, 5 * bound // 2), :]

    def merge(c):
        s = c % 2
        await_bytes(q_bytes(s), qrecv.at[s])
        if nz < NC:
            @pl.when(c >= nz)
            def _():
                await_bytes(zs.at[c % nz], zsend.at[c % nz])
        zs[c % nz] = zq[s, :3 * bound, mine] + zin[s]
        recv[c, pl.ds(chip * bound, bound), :] = zq[s, 3 * bound:, :] + zown[s]
        for n, dev in ((2, dg), (0, xn), (1, yn)):
            z_copy(c, n, dev).start()

    def forward(c):
        await_bytes(zs.at[0], zrecv.at[c])
        for d in far:
            fwd_copy(c, d).start()

    def second_product(c, _):
        def group(g, _):
            i = c * groups + 2 * g
            w2_copy(i).wait()
            w2_copy(i + 1).wait()
            for j in range(2 * ge):
                rows = pl.ds(g * (2 * ge * CAP) + j * CAP, CAP)
                zc_s[rows, :] = dot(h_s[rows, :], w2buf[(i + j // ge) % ns2, j % ge]).astype(BF16)

            for n in (i, i + 1):
                @pl.when(n + ns2 < items)
                def _():
                    w2_copy(n + ns2).start()

            return 0

        lax.fori_loop(0, groups // 2, group, 0)
        @pl.when(c > 1)
        def _():
            await_bytes(q_bytes(c % 2), qsend.at[c % 2])

        zq[c % 2] = dot(q_s[...], zc_s[...]).astype(BF16)
        for copy in q_copies(c % 2):
            copy.start()

        @pl.when(c < turns)
        def _():
            lax.fori_loop(c * per, (c + 1) * per, build_a, 0)

        merge(c)

        @pl.when(c > 3)
        def _():
            forward(c - 4)

        return 0

    lax.fori_loop(0, NC, second_product, 0)
    def cut_a(j, _):
        a = at_s[pl.ds(j * 128, 128), :].T
        for n in range(3):
            part = a.astype(BF16)
            a_s[n, :, pl.ds(j * 128, 128)] = part
            a = a - part.astype(F32)
        return 0

    lax.fori_loop(0, rows_in // 128, cut_a, 0)

    def out_copy(c):
        return pltpu.make_async_copy(out_s.at[c], out.at[:, pl.ds(c * CW, CW)], osem)

    def combine(c):
        recv_half = recv.at[c, pl.ds(0, 3 * bound), pl.ds(0, HW)]
        await_bytes(recv_half, zfrecv.at[c])
        z = recv[c]
        y = dot(a_s[2], z) + dot(a_s[1], z) + dot(a_s[0], z)
        out_s[c] = (xr[c, pl.ds(k * TOK, TOK), :].astype(F32) + y).astype(BF16)
        out_copy(c).start()

    def step(c, _):
        for at, chunk_in in ((1, 5), (6, 6), (6, 7)):
            @pl.when(c == at)
            def _():
                forward(chunk_in)

        combine(c)
        return 0

    await_bytes(seven, csend)
    await_bytes(seven, ksend)
    await_bytes(out_s, psend)
    await_bytes(xs, xsend)
    await_bytes(xs, xfsend)
    forward(4)
    lax.fori_loop(0, NC, step, 0)
    for s in range(2):
        await_bytes(q_bytes(s), qsend.at[s])
    for s in range(nz):
        await_bytes(zs.at[s], zsend.at[s])
    await_bytes(recv.at[:, pl.ds(0, 3 * bound), pl.ds(0, HW)], zfsend)
    await_bytes(out_s, osem)


def moe_call(xb, bound, ge, ns1, ns2, nz, cid, tok, logit, w1, w2):
    nx = -(-(2 * TOK + 6 * xb) // 128) * 128
    rows_in = -(-4 * bound // 128) * 128
    vm = pltpu.VMEM
    sem = pltpu.SemaphoreType.DMA
    sq = vm((ALL_EXP, TOK), F32)
    return pl.pallas_call(
        functools.partial(moe_kernel, xb, nx, bound, ge, ns1, ns2, nz),
        out_shape=(jax.ShapeDtypeStruct((TOK, D), BF16), jax.ShapeDtypeStruct((1, 1), jnp.int32)),
        in_specs=[pl.BlockSpec(memory_space=pl.ANY)] * 4,
        out_specs=(pl.BlockSpec(memory_space=pl.ANY), pl.BlockSpec(memory_space=pltpu.SMEM)),
        scratch_shapes=[
            vm((NC, nx, CW), BF16), vm((NC, 3 * xb, CW), BF16),
            vm((ns1, ge, CW, FF), BF16), vm((ns2, ge, FF, CW), BF16),
            sq, vm((8, ALL_EXP), F32), vm((64, ALL_EXP), F32), vm((8, ALL_EXP), F32), vm((64, ALL_EXP), F32),
            vm((16, TOK), F32), vm((3 * xb, TOK), BF16), sq,
            vm((SLOTS, nx), BF16), vm((SLOTS, 128), F32), vm((8, SLOTS), F32), vm((4 * bound, SLOTS), BF16),
            vm((SLOTS, CW), BF16), vm((SLOTS, FF), F32), vm((SLOTS, FF), BF16), vm((SLOTS, CW), BF16),
            vm((2, 4 * bound, CW), BF16), vm((2, 3 * bound, HW), BF16), vm((2, bound, CW), BF16),
            vm((nz, 3 * bound, HW), BF16), vm((NC, rows_in, CW), BF16),
            sq, sq, vm((rows_in, TOK), F32), vm((3, TOK, rows_in), BF16), vm((NC, TOK, CW), BF16),
            sem((ns1,)), sem((ns2,)), *[sem] * 11, sem((NC,)), sem((NC,)),
            sem((nz,)), sem, sem((NC,)), sem((NC,)), sem((2,)), sem((2,)),
        ],
        compiler_params=pltpu.CompilerParams(collective_id=cid, has_side_effects=True, vmem_limit_bytes=67043328),
        name=f"moe_{bound}",
    )(tok, logit, w1, w2)


def solution(mesh):
    row_spec = P(("dp", "ep"), None)
    expert_spec = P("ep", None, None)

    def device_step(tok, logit, w1, w2):
        out, flag = moe_call(144, 336, 8, 8, 8, NC, 0, tok, logit, w1, w2)
        return lax.switch(flag[0, 0], (lambda: out, lambda: moe_call(TOK, 1024, 2, 2, 2, 2, 1, tok, logit, w1, w2)[0]))

    return jax.shard_map(device_step, mesh=mesh, in_specs=(row_spec, row_spec, expert_spec, expert_spec),
                         out_specs=row_spec, check_vma=False)
```

```python
import functools

import jax
import jax.numpy as jnp
from jax import lax
from jax.experimental import pallas as pl
from jax.experimental.pallas import tpu as pltpu
from jax.sharding import PartitionSpec as P

MESH = pl.DeviceIdType.MESH
F32, BF16 = jnp.float32, jnp.bfloat16
DEV = 8
TOK = 256
D = 2048
FF = 512
EXP = 32
ALL_EXP = EXP * DEV
CAP = 16
SLOTS = EXP * CAP
NC = 8
CW = D // NC
HW = CW // 2


def dot(a, b):
    return jnp.dot(a, b, preferred_element_type=F32)


def iota(shape, dim):
    return lax.broadcasted_iota(jnp.int32, shape, dim)


def gelu(v):
    return 0.5 * v * (1.0 + lax.erf(v * 0.7071067811865476))


def dot_nt(a, b):
    return lax.dot_general(a, b, (((1,), (1,)), ((), ())), preferred_element_type=F32)


def onehot(cond):
    return jnp.where(cond, 1.0, 0.0).astype(BF16)


def moe_kernel(xb, nx, bound, ge, ns1, ns2, nz, lag, tok, logit, w1, w2, out, flag_out,
               xo, xl, xq, xin, xs, plog, w1buf, w2buf, log_s, cand, cands, rk, rks, rt_s, w_s, c64_s,
               p_s, v_s, vt_s, q_s, pick_s, own_s, hacc, h_s, zc_s, zq, zin, zown, zs, recv,
               r2_s, gt_s, at_s, a_s, out_s,
               w1sem, w2sem, xsem, osem, lsem, csend, crecv, ksend, krecv, xsend, xfsend, psend, precv, xrecv, xfrecv,
               zsend, zfsend, zrecv, zfrecv, qsend, qrecv, xqsend, xqrecv, gsend, grecv):
    groups = EXP // ge
    items = NC * groups
    rows_in = recv.shape[2]
    ahead_of = own_s.shape[0] == NC
    me = lax.axis_index("ep")
    k = me % 2
    chip = me // 2
    cx = chip % 2
    cy = chip // 2
    dx = 2 - 4 * cx
    dy = 4 - 8 * cy
    other = 1 - 2 * k
    partner = me + other
    xn, yn, dg = me + dx, me + dy, me + dx + dy
    far = (xn, yn, dg)
    neg = jnp.float32(-jnp.inf)

    def rcopy(src, dst, ss, rs, dev):
        return pltpu.make_async_remote_copy(src_ref=src, dst_ref=dst, send_sem=ss, recv_sem=rs,
                                            device_id={"ep": dev}, device_id_type=MESH)

    def w1_copy(i):
        s = i % ns1
        return pltpu.make_async_copy(
            w1.at[pl.ds((i % groups) * ge, ge), pl.ds((i // groups) * CW, CW), :], w1buf.at[s], w1sem.at[s])

    def w2_copy(i):
        s = i % ns2
        return pltpu.make_async_copy(
            w2.at[pl.ds((i % groups) * ge, ge), :, pl.ds((i // groups) * CW, CW)], w2buf.at[s], w2sem.at[s])

    def xown(c, core):
        return xo.at[c, pl.ds(core * TOK, TOK), :]

    def x_copy(c):
        return pltpu.make_async_copy(tok.at[:, pl.ds(c * CW, CW)], xown(c, k), xsem)

    def await_bytes(ref, sem):
        pltpu.make_async_copy(ref, ref, sem).wait()

    def p_copy(c):
        return rcopy(xown(c, k), xown(c, k), psend, precv, partner)

    def x_send(c, n):
        part = pl.ds(n * xb, xb)
        s = c % nz
        return rcopy(xs.at[s, part, :], xl.at[c, k, part, :], xsend.at[s], xrecv.at[c], far[n])

    def x_fwd(c):
        return rcopy(xl.at[c, k], xl.at[c, k], xfsend, xfrecv.at[c], partner)

    def x_swap(s):
        return rcopy(xq.at[s, 1 - k], xin.at[s], xqsend.at[s], xqrecv.at[s], partner)

    log_copy = pltpu.make_async_copy(logit, log_s, lsem)
    log_copy.start()
    barrier = pltpu.get_barrier_semaphore()
    for j in range(1, DEV):
        pl.semaphore_signal(barrier, inc=1, device_id={"ep": (me + j) % DEV}, device_id_type=MESH)
    for c in range(NC):
        x_copy(c).start()
    log_copy.wait()

    def next_top(n, m):
        v = log_s[...]
        m = jnp.max(jnp.where(v < m, v, neg), axis=0, keepdims=True)
        cand[pl.ds(n, 1), :] = m
        return m

    lax.fori_loop(0, 8, next_top, jnp.full((1, ALL_EXP), jnp.inf, F32))
    pl.semaphore_wait(barrier, DEV - 1)

    def c_copy(j):
        return rcopy(cand, cands.at[pl.ds(me * 8, 8), :], csend, crecv, (me + j) % DEV)

    def k_copy(j):
        return rcopy(rk, rks.at[pl.ds(me * 8, 8), :], ksend, krecv, (me + j) % DEV)

    log_swap = rcopy(log_s, plog, gsend, grecv, partner)
    seven = cands.at[pl.ds(0, 8 * (DEV - 1)), :]
    for j in range(1, DEV):
        c_copy(j).start()
    log_swap.start()
    cands[pl.ds(me * 8, 8), :] = cand[...]

    await_bytes(out_s, xsem)
    for c in range(NC):
        p_copy(c).start()
    if rows_in > 4 * bound:
        for c in range(NC):
            recv[c, :, 4 * bound:, :] = jnp.zeros((2, rows_in - 4 * bound, HW), BF16)
        at_s[4 * bound:, :] = jnp.zeros((rows_in - 4 * bound, TOK), F32)
    for i in range(ns1):
        w1_copy(i).start()
    for i in range(ns2):
        w2_copy(i).start()
    t0, t1 = iota((TOK, TOK), 0), iota((TOK, TOK), 1)
    tri = onehot(t0 < t1)
    await_bytes(seven, crecv)
    log_swap.wait_recv()

    def next_max(_, m):
        v = cands[...]
        return jnp.max(jnp.where(v < m, v, neg), axis=0, keepdims=True)

    thr = lax.fori_loop(0, CAP, next_max, jnp.full((1, ALL_EXP), jnp.inf, F32))

    core = k.astype(F32)
    mo = onehot(log_s[...] >= thr)
    mp = onehot(plog[...] >= thr)
    of_chip = onehot((iota((16, ALL_EXP), 1) >> 6) == iota((16, ALL_EXP), 0))
    used = dot_nt(of_chip, mo) > 0.5
    ahead = core * jnp.sum(jnp.where(dot_nt(of_chip, mp) > 0.5, 1.0, 0.0), axis=1, keepdims=True)
    rt_s[...] = jnp.where(used, dot(onehot(used), tri) + ahead, -1.0)
    xio = iota((xb, TOK), 0).astype(F32)
    for n in range(3):
        w_s[n * xb:(n + 1) * xb, :] = onehot(rt_s[pl.ds(far[n] // 2, 1), :] == xio)

    nq = 2 * lag

    def compact(c):
        s = c % nq
        new = dot(w_s[...], xo[c, pl.ds(k * TOK, TOK), :]).astype(BF16)
        xq[s, 0] = new[:, :HW]
        xq[s, 1] = new[:, HW:]
        x_swap(s).start()

    def x_merge(c):
        s = c % nq
        await_bytes(xin.at[s], xqrecv.at[s])
        if nz < NC and isinstance(c, int):
            await_bytes(xs.at[c % nz], xsend.at[c % nz])
        elif nz < NC:
            @pl.when(c >= nz)
            def _():
                await_bytes(xs.at[c % nz], xsend.at[c % nz])
        xs[c % nz] = xq[s, k] + xin[s]
        for n in (2, 0, 1):
            x_send(c, n).start()

    for c in range(lag):
        compact(c)

    of_chip2 = onehot((iota((ALL_EXP, 128), 0) >> 6) == iota((ALL_EXP, 128), 1))
    used2 = onehot(dot(mo, of_chip2) > 0.5)
    place = dot(onehot(t1 < t0), used2)
    place = jnp.where(iota((TOK, 128), 1) == chip, iota((TOK, 128), 0).astype(F32), place)
    used_p = jnp.where(dot(mp, of_chip2) > 0.5, 1.0, 0.0)
    shift = core * jnp.sum(used_p, axis=0, keepdims=True)
    shift = jnp.broadcast_to(jnp.where(iota((1, 128), 1) == chip, 0.0, shift), (8, 128))
    shift = dot_nt(shift.astype(BF16), of_chip2)
    c64_s[...] = dot_nt(place.astype(BF16), of_chip2) + shift[:1, :]

    def top_place(n, _):
        hit = log_s[...] == cand[pl.ds(n, 1), :]
        rk[pl.ds(n, 1), :] = jnp.max(jnp.where(hit, c64_s[...], -1.0), axis=0, keepdims=True)
        return 0

    lax.fori_loop(0, 8, top_place, 0)
    for j in range(1, DEV):
        k_copy(j).start()
    rks[pl.ds(me * 8, 8), :] = rk[...]
    def exchange(c, _):
        x_merge(c - lag)

        @pl.when(c >= nq)
        def _():
            await_bytes(xin.at[c % nq], xqsend.at[c % nq])

        compact(c)
        return 0

    lax.fori_loop(lag, NC, exchange, 0)
    for c in range(NC - lag, NC):
        x_merge(c)

    cv = cands[...]
    sel = cv >= thr
    so = onehot(sel)
    j0, j1 = iota((64, 64), 0), iota((64, 64), 1)
    slot = dot(onehot(j1 < j0), so)
    inside = dot(onehot((j1 < j0) & ((j1 >> 4) == (j0 >> 4))), so)
    num = dot(onehot((j1 >> 4) == (j0 >> 4)), so)
    base = dot(num.astype(BF16), onehot((t0 < t1) & ((t0 >> 6) == (t1 >> 6))))
    rank = base + inside
    over = jnp.max(jnp.max(base + num, axis=0, keepdims=True), axis=1, keepdims=True) > bound
    c64_s[:64, :] = jnp.where(sel, rank, -1.0)

    pair = jnp.full((TOK, ALL_EXP), -1.0, F32)
    for n in range(8):
        pair = jnp.where(log_s[...] == cand[n:n + 1, :], c64_s[pl.ds(me * 8 + n, 1), :], pair)
    r2_s[...] = pair.T
    la = log_s[...].T
    ex = jnp.exp(la - jnp.max(la, axis=0, keepdims=True))
    gt_s[...] = ex / jnp.sum(ex, axis=0, keepdims=True)

    await_bytes(seven, krecv)
    rv = rks[...]
    src = iota((64, ALL_EXP), 0) >> 3
    exp_chip = iota((64, ALL_EXP), 1) >> 6
    wide = jnp.max(jnp.max(jnp.where(sel & ((src >> 1) != exp_chip), rv, -1.0), axis=0, keepdims=True),
                   axis=1, keepdims=True) >= xb
    flag_out[0, 0] = jnp.max(jnp.where(over | wide, 1.0, 0.0)).astype(jnp.int32)
    rel = (src >> 1) ^ chip
    start = jnp.where(rel == 0, (src & 1) * TOK, 2 * TOK + (rel - 1) * xb).astype(F32)
    pos = start + rv + 1.0
    code = ((src >> 1) * 1024).astype(F32) + rank + 1.0
    pos_rows, code_rows = [], []
    for i in range(CAP):
        hit = sel & (slot == i)
        pos_rows.append(jnp.sum(jnp.where(hit, pos, 0.0), axis=0, keepdims=True))
        code_rows.append(jnp.sum(jnp.where(hit, code, 0.0), axis=0, keepdims=True))
    turn = ALL_EXP - me * EXP
    pos = pltpu.roll(jnp.concatenate(pos_rows, axis=0), turn, 1)
    code = pltpu.roll(jnp.concatenate(code_rows, axis=0), turn, 1)
    pio = iota((CAP, nx), 1).astype(F32) + 1.0
    for e in range(EXP):
        p_s[e * CAP:(e + 1) * CAP, :] = onehot(pos[:, e:e + 1] == pio)
        v_s[e * CAP:(e + 1) * CAP, :] = jnp.broadcast_to(code[:, e:e + 1], (CAP, 128))
    vt_s[...] = v_s[...].T[:8, :]
    rio = iota((bound, SLOTS), 0)
    for n, d in enumerate((xn, yn, dg, me)):
        want = (rio + ((d // 2) * 1024 + 1)).astype(F32)
        q_s[n * bound:(n + 1) * bound, :] = onehot(vt_s[0:1, :] == want)
    hacc[...] = jnp.zeros((SLOTS, FF), F32)

    def x_forward(c):
        await_bytes(xs.at[0], xrecv.at[c])
        x_fwd(c).start()

    def first_product(c, last):
        await_bytes(xs.at[0], xfrecv.at[c])
        lists = jnp.concatenate([xl[c, 0], xl[c, 1]], axis=1)
        near = own_s[c] if ahead_of else dot(p_s[:, :2 * TOK], xo[c])
        pick_s[...] = (near + dot(p_s[:, 2 * TOK:], lists)).astype(BF16)

        def group(g, _):
            i = c * groups + 2 * g
            w1_copy(i).wait()
            w1_copy(i + 1).wait()
            for j in range(2 * ge):
                rows = pl.ds(g * (2 * ge * CAP) + j * CAP, CAP)
                v = hacc[rows, :] + dot(pick_s[rows, :], w1buf[(i + j // ge) % ns1, j % ge])
                if last:
                    h_s[rows, :] = gelu(v).astype(BF16)
                else:
                    hacc[rows, :] = v

            for n in (i, i + 1):
                @pl.when(n + ns1 < items)
                def _():
                    w1_copy(n + ns1).start()

            return 0

        lax.fori_loop(0, groups // 2, group, 0)

    def chunk(c, _):
        x_forward(c + 1)
        first_product(c, False)
        return 0

    await_bytes(out_s, precv)
    x_forward(0)

    def pick_own(c, _):
        own_s[c] = dot(p_s[:, :2 * TOK], xo[c]).astype(BF16)
        return 0

    if ahead_of:
        lax.fori_loop(0, NC, pick_own, 0)
    lax.fori_loop(0, NC - 1, chunk, 0)
    first_product(NC - 1, True)

    RB = 64 if bound % 64 == 0 else 48

    def build_a(n, _):
        o = n // (bound // RB)
        r0 = (n % (bound // RB)) * RB
        rio2 = (iota((RB, TOK), 0) + r0).astype(F32)

        def one(e, acc):
            row = pl.ds(o * 2 * EXP + e, 1)
            return jnp.where(r2_s[row, :] == rio2, gt_s[row, :], acc)

        at_s[pl.ds(o * bound + r0, RB), :] = lax.fori_loop(0, 2 * EXP, one, jnp.zeros((RB, TOK), F32), unroll=8)
        return 0

    blocks = 4 * (bound // RB)
    per = blocks // NC + (blocks % NC > 0)

    def rblk(c, d):
        return recv.at[c, k, pl.ds((d // 2) * bound, bound), :]

    def q_copies(s):
        return (rcopy(zq.at[s, 1 - k], zin.at[s], qsend.at[s], qrecv.at[s], partner),
                rcopy(zq.at[s, k, pl.ds(3 * bound, bound), :], zown.at[s], qsend.at[s], qrecv.at[s], partner))

    def z_copy(c, n, dev):
        return rcopy(zs.at[c % nz, pl.ds(n * bound, bound), :], rblk(c, me), zsend.at[c % nz], zrecv.at[c], dev)

    def fwd_copy(c, d):
        return rcopy(rblk(c, d), rblk(c, d), zfsend, zfrecv.at[c], partner)

    def q_bytes(s):
        return zq.at[s, :, pl.ds(0, 5 * bound // 2), :]

    def merge(c):
        s = c % 2
        await_bytes(q_bytes(s), qrecv.at[s])
        if nz < NC:
            @pl.when(c >= nz)
            def _():
                await_bytes(zs.at[c % nz], zsend.at[c % nz])
        zs[c % nz] = zq[s, k, :3 * bound, :] + zin[s, :3 * bound, :]
        home = pl.ds(chip * bound, bound)
        recv[c, k, home, :] = zq[s, k, 3 * bound:, :] + zin[s, 3 * bound:, :]
        recv[c, 1 - k, home, :] = zq[s, 1 - k, 3 * bound:, :] + zown[s]
        for n, dev in ((2, dg), (0, xn), (1, yn)):
            z_copy(c, n, dev).start()

    def forward(c):
        await_bytes(zs.at[0], zrecv.at[c])
        for d in far:
            fwd_copy(c, d).start()

    def second_product(c, _):
        def group(g, _):
            i = c * groups + 2 * g
            w2_copy(i).wait()
            w2_copy(i + 1).wait()
            for j in range(2 * ge):
                rows = pl.ds(g * (2 * ge * CAP) + j * CAP, CAP)
                zc_s[rows, :] = dot(h_s[rows, :], w2buf[(i + j // ge) % ns2, j % ge]).astype(BF16)

            for n in (i, i + 1):
                @pl.when(n + ns2 < items)
                def _():
                    w2_copy(n + ns2).start()

            return 0

        lax.fori_loop(0, groups // 2, group, 0)
        @pl.when(c > 1)
        def _():
            merge(c - 1)
            await_bytes(q_bytes(c % 2), qsend.at[c % 2])

        zq_new = dot(q_s[...], zc_s[...]).astype(BF16)
        zq[c % 2, 0] = zq_new[:, :HW]
        zq[c % 2, 1] = zq_new[:, HW:]
        for copy in q_copies(c % 2):
            copy.start()

        @pl.when(c == 0)
        def _():
            merge(0)

        @pl.when(c > 1)
        def _():
            lax.fori_loop((c - 2) * per, (c - 1) * per, build_a, 0)

        @pl.when(c > 3)
        def _():
            forward(c - 4)

        return 0

    lax.fori_loop(0, NC, second_product, 0)
    merge(NC - 1)
    lax.fori_loop((NC - 2) * per, blocks, build_a, 0)
    def cut_a(j, _):
        a = at_s[pl.ds(j * 128, 128), :].T
        for n in range(3):
            part = a.astype(BF16)
            a_s[n, :, pl.ds(j * 128, 128)] = part
            a = a - part.astype(F32)
        return 0

    lax.fori_loop(0, rows_in // 128, cut_a, 0)

    def out_copy(c):
        return pltpu.make_async_copy(out_s.at[c], out.at[:, pl.ds(c * CW, CW)], osem)

    def combine(c):
        await_bytes(recv.at[c, 0, pl.ds(0, 3 * bound), :], zfrecv.at[c])
        z = jnp.concatenate([recv[c, 0], recv[c, 1]], axis=1)
        y = dot(a_s[2], z) + dot(a_s[1], z) + dot(a_s[0], z)
        out_s[c] = (xo[c, pl.ds(k * TOK, TOK), :].astype(F32) + y).astype(BF16)
        out_copy(c).start()

    def step(c, _):
        for at, chunk_in in ((1, 5), (6, 6), (6, 7)):
            @pl.when(c == at)
            def _():
                forward(chunk_in)

        combine(c)
        return 0

    await_bytes(seven, csend)
    await_bytes(seven, ksend)
    await_bytes(out_s, psend)
    for s in range(nz):
        await_bytes(xs.at[s], xsend.at[s])
    await_bytes(xl.at[:, 0], xfsend)
    forward(4)
    lax.fori_loop(0, NC, step, 0)
    log_swap.wait_send()
    for s in range(nq):
        await_bytes(xin.at[s], xqsend.at[s])
    for s in range(2):
        await_bytes(q_bytes(s), qsend.at[s])
    for s in range(nz):
        await_bytes(zs.at[s], zsend.at[s])
    await_bytes(recv.at[:, 0, pl.ds(0, 3 * bound), :], zfsend)
    await_bytes(out_s, osem)


def moe_call(xb, bound, ge, ns1, ns2, nz, lag, cid, tok, logit, w1, w2):
    nx = 2 * TOK + 3 * xb
    rows_in = -(-4 * bound // 128) * 128
    vm = pltpu.VMEM
    sem = pltpu.SemaphoreType.DMA
    sq = vm((ALL_EXP, TOK), F32)
    return pl.pallas_call(
        functools.partial(moe_kernel, xb, nx, bound, ge, ns1, ns2, nz, lag),
        out_shape=(jax.ShapeDtypeStruct((TOK, D), BF16), jax.ShapeDtypeStruct((1, 1), jnp.int32)),
        in_specs=[pl.BlockSpec(memory_space=pl.ANY)] * 4,
        out_specs=(pl.BlockSpec(memory_space=pl.ANY), pl.BlockSpec(memory_space=pltpu.SMEM)),
        scratch_shapes=[
            vm((NC, 2 * TOK, CW), BF16), vm((NC, 2, 3 * xb, HW), BF16), vm((2 * lag, 2, 3 * xb, HW), BF16),
            vm((2 * lag, 3 * xb, HW), BF16), vm((nz, 3 * xb, HW), BF16), sq,
            vm((ns1, ge, CW, FF), BF16), vm((ns2, ge, FF, CW), BF16),
            sq, vm((8, ALL_EXP), F32), vm((64, ALL_EXP), F32), vm((8, ALL_EXP), F32), vm((64, ALL_EXP), F32),
            vm((16, TOK), F32), vm((3 * xb, TOK), BF16), sq,
            vm((SLOTS, nx), BF16), vm((SLOTS, 128), F32), vm((8, SLOTS), F32), vm((4 * bound, SLOTS), BF16),
            vm((SLOTS, CW), BF16), vm((nz, SLOTS, CW), BF16), vm((SLOTS, FF), F32), vm((SLOTS, FF), BF16), vm((SLOTS, CW), BF16),
            vm((2, 2, 4 * bound, HW), BF16), vm((2, 4 * bound, HW), BF16), vm((2, bound, HW), BF16),
            vm((nz, 3 * bound, HW), BF16), vm((NC, 2, rows_in, HW), BF16),
            sq, sq, vm((rows_in, TOK), F32), vm((3, TOK, rows_in), BF16), vm((NC, TOK, CW), BF16),
            sem((ns1,)), sem((ns2,)), *[sem] * 7, sem((nz,)), *[sem] * 3, sem((NC,)), sem((NC,)),
            sem((nz,)), sem, sem((NC,)), sem((NC,)), sem((2,)), sem((2,)), sem((2 * lag,)), sem((2 * lag,)), sem, sem,
        ],
        compiler_params=pltpu.CompilerParams(collective_id=cid, has_side_effects=True, vmem_limit_bytes=67043328),
        name=f"moe_{bound}",
    )(tok, logit, w1, w2)


def solution(mesh):
    row_spec = P(("dp", "ep"), None)
    expert_spec = P("ep", None, None)

    def device_step(tok, logit, w1, w2):
        out, flag = moe_call(256, 336, 8, 7, 7, NC, 2, 0, tok, logit, w1, w2)
        return lax.switch(flag[0, 0], (lambda: out, lambda: moe_call(2 * TOK, 1024, 1, 2, 2, 1, 1, 1, tok, logit, w1, w2)[0]))

    return jax.shard_map(device_step, mesh=mesh, in_specs=(row_spec, row_spec, expert_spec, expert_spec),
                         out_specs=row_spec, check_vma=False)
```

```python
import functools

import jax
import jax.numpy as jnp
from jax import lax
from jax.experimental import pallas as pl
from jax.experimental.pallas import tpu as pltpu
from jax.sharding import PartitionSpec as P

MESH = pl.DeviceIdType.MESH
F32, BF16 = jnp.float32, jnp.bfloat16
DEV = 8
TOK = 256
D = 2048
FF = 512
EXP = 32
ALL_EXP = EXP * DEV
CAP = 16
SLOTS = EXP * CAP
NC = 8
CW = D // NC
HW = CW // 2


def dot(a, b):
    return jnp.dot(a, b, preferred_element_type=F32)


def iota(shape, dim):
    return lax.broadcasted_iota(jnp.int32, shape, dim)


def gelu(v):
    return 0.5 * v * (1.0 + lax.erf(v * 0.7071067811865476))


def dot_nt(a, b):
    return lax.dot_general(a, b, (((1,), (1,)), ((), ())), preferred_element_type=F32)


def onehot(cond):
    return jnp.where(cond, 1.0, 0.0).astype(BF16)


def moe_kernel(xb, nx, bound, ge, ns1, ns2, nz, lag, tok, logit, w1, w2, out, flag_out,
               xo, xl, xq, xin, xs, plog, w1buf, w2buf, log_s, cand, cands, rk, rks, rt_s, w_s, c64_s,
               p_s, v_s, vt_s, q_s, pick_s, own_s, hacc, h_s, zc_s, zq, zin, zown, zs, recv,
               r2_s, gt_s, at_s, a_s, out_s,
               w1sem, w2sem, xsem, osem, lsem, csend, crecv, ksend, krecv, xsend, xfsend, psend, precv, xrecv, xfrecv,
               zsend, zfsend, zrecv, zfrecv, qsend, qrecv, xqsend, xqrecv, gsend, grecv):
    groups = EXP // ge
    items = NC * groups
    rows_in = recv.shape[2]
    ahead_of = own_s.shape[0] == NC
    me = lax.axis_index("ep")
    k = me % 2
    chip = me // 2
    cx = chip % 2
    cy = chip // 2
    dx = 2 - 4 * cx
    dy = 4 - 8 * cy
    other = 1 - 2 * k
    partner = me + other
    xn, yn, dg = me + dx, me + dy, me + dx + dy
    far = (xn, yn, dg)
    neg = jnp.float32(-jnp.inf)

    def rcopy(src, dst, ss, rs, dev):
        return pltpu.make_async_remote_copy(src_ref=src, dst_ref=dst, send_sem=ss, recv_sem=rs,
                                            device_id={"ep": dev}, device_id_type=MESH)

    def w1_copy(i):
        s = i % ns1
        return pltpu.make_async_copy(
            w1.at[pl.ds((i % groups) * ge, ge), pl.ds((i // groups) * CW, CW), :], w1buf.at[s], w1sem.at[s])

    def w2_copy(i):
        s = i % ns2
        return pltpu.make_async_copy(
            w2.at[pl.ds((i % groups) * ge, ge), :, pl.ds((i // groups) * CW, CW)], w2buf.at[s], w2sem.at[s])

    def xown(c, core):
        return xo.at[c, pl.ds(core * TOK, TOK), :]

    def x_copy(c):
        return pltpu.make_async_copy(tok.at[:, pl.ds(c * CW, CW)], xown(c, k), xsem)

    def await_bytes(ref, sem):
        pltpu.make_async_copy(ref, ref, sem).wait()

    def p_copy(c):
        return rcopy(xown(c, k), xown(c, k), psend, precv, partner)

    def x_send(c, n):
        part = pl.ds(n * xb, xb)
        s = c % nz
        return rcopy(xs.at[s, part, :], xl.at[c, k, part, :], xsend.at[s], xrecv.at[c], far[n])

    def x_fwd(c):
        return rcopy(xl.at[c, k], xl.at[c, k], xfsend, xfrecv.at[c], partner)

    def x_swap(s):
        return rcopy(xq.at[s, 1 - k], xin.at[s], xqsend.at[s], xqrecv.at[s], partner)

    log_copy = pltpu.make_async_copy(logit, log_s, lsem)
    log_copy.start()
    barrier = pltpu.get_barrier_semaphore()
    for j in range(1, DEV):
        pl.semaphore_signal(barrier, inc=1, device_id={"ep": (me + j) % DEV}, device_id_type=MESH)
    for c in range(NC):
        x_copy(c).start()
    log_copy.wait()

    def next_top(n, m):
        v = log_s[...]
        m = jnp.max(jnp.where(v < m, v, neg), axis=0, keepdims=True)
        cand[pl.ds(n, 1), :] = m
        return m

    lax.fori_loop(0, 8, next_top, jnp.full((1, ALL_EXP), jnp.inf, F32))
    pl.semaphore_wait(barrier, DEV - 1)

    def c_copy(j):
        return rcopy(cand, cands.at[pl.ds(me * 8, 8), :], csend, crecv, (me + j) % DEV)

    def k_copy(j):
        return rcopy(rk, rks.at[pl.ds(me * 8, 8), :], ksend, krecv, (me + j) % DEV)

    log_swap = rcopy(log_s, plog, gsend, grecv, partner)
    seven = cands.at[pl.ds(0, 8 * (DEV - 1)), :]
    for j in range(1, DEV):
        c_copy(j).start()
    log_swap.start()
    cands[pl.ds(me * 8, 8), :] = cand[...]

    await_bytes(out_s, xsem)
    for c in range(NC):
        p_copy(c).start()
    if rows_in > 4 * bound:
        for c in range(NC):
            recv[c, :, 4 * bound:, :] = jnp.zeros((2, rows_in - 4 * bound, HW), BF16)
        at_s[4 * bound:, :] = jnp.zeros((rows_in - 4 * bound, TOK), F32)
    for i in range(ns1):
        w1_copy(i).start()
    for i in range(ns2):
        w2_copy(i).start()
    t0, t1 = iota((TOK, TOK), 0), iota((TOK, TOK), 1)
    tri = onehot(t0 < t1)
    await_bytes(seven, crecv)
    log_swap.wait_recv()

    def next_max(_, m):
        v = cands[...]
        return jnp.max(jnp.where(v < m, v, neg), axis=0, keepdims=True)

    thr = lax.fori_loop(0, CAP, next_max, jnp.full((1, ALL_EXP), jnp.inf, F32))

    core = k.astype(F32)
    mo = onehot(log_s[...] >= thr)
    mp = onehot(plog[...] >= thr)
    of_chip = onehot((iota((16, ALL_EXP), 1) >> 6) == iota((16, ALL_EXP), 0))
    used = dot_nt(of_chip, mo) > 0.5
    ahead = core * jnp.sum(jnp.where(dot_nt(of_chip, mp) > 0.5, 1.0, 0.0), axis=1, keepdims=True)
    rt_s[...] = jnp.where(used, dot(onehot(used), tri) + ahead, -1.0)
    xio = iota((xb, TOK), 0).astype(F32)
    for n in range(3):
        w_s[n * xb:(n + 1) * xb, :] = onehot(rt_s[pl.ds(far[n] // 2, 1), :] == xio)

    nq = 2 * lag

    def compact(c):
        s = c % nq
        new = dot(w_s[...], xo[c, pl.ds(k * TOK, TOK), :]).astype(BF16)
        xq[s, 0] = new[:, :HW]
        xq[s, 1] = new[:, HW:]
        x_swap(s).start()

    def x_merge(c):
        s = c % nq
        await_bytes(xin.at[s], xqrecv.at[s])
        if nz < NC and isinstance(c, int):
            await_bytes(xs.at[c % nz], xsend.at[c % nz])
        elif nz < NC:
            @pl.when(c >= nz)
            def _():
                await_bytes(xs.at[c % nz], xsend.at[c % nz])
        xs[c % nz] = xq[s, k] + xin[s]
        for n in (2, 0, 1):
            x_send(c, n).start()

    for c in range(lag):
        compact(c)

    of_chip2 = onehot((iota((ALL_EXP, 128), 0) >> 6) == iota((ALL_EXP, 128), 1))
    used2 = onehot(dot(mo, of_chip2) > 0.5)
    place = dot(onehot(t1 < t0), used2)
    place = jnp.where(iota((TOK, 128), 1) == chip, iota((TOK, 128), 0).astype(F32), place)
    used_p = jnp.where(dot(mp, of_chip2) > 0.5, 1.0, 0.0)
    shift = core * jnp.sum(used_p, axis=0, keepdims=True)
    shift = jnp.broadcast_to(jnp.where(iota((1, 128), 1) == chip, 0.0, shift), (8, 128))
    shift = dot_nt(shift.astype(BF16), of_chip2)
    c64_s[...] = dot_nt(place.astype(BF16), of_chip2) + shift[:1, :]

    def top_place(n, _):
        hit = log_s[...] == cand[pl.ds(n, 1), :]
        rk[pl.ds(n, 1), :] = jnp.max(jnp.where(hit, c64_s[...], -1.0), axis=0, keepdims=True)
        return 0

    lax.fori_loop(0, 8, top_place, 0)
    for j in range(1, DEV):
        k_copy(j).start()
    rks[pl.ds(me * 8, 8), :] = rk[...]
    def exchange(c, _):
        x_merge(c - lag)

        @pl.when(c >= nq)
        def _():
            await_bytes(xin.at[c % nq], xqsend.at[c % nq])

        compact(c)
        return 0

    lax.fori_loop(lag, NC, exchange, 0)
    for c in range(NC - lag, NC):
        x_merge(c)

    cv = cands[...]
    sel = cv >= thr
    so = onehot(sel)
    j0, j1 = iota((64, 64), 0), iota((64, 64), 1)
    slot = dot(onehot(j1 < j0), so)
    inside = dot(onehot((j1 < j0) & ((j1 >> 4) == (j0 >> 4))), so)
    num = dot(onehot((j1 >> 4) == (j0 >> 4)), so)
    base = dot(num.astype(BF16), onehot((t0 < t1) & ((t0 >> 6) == (t1 >> 6))))
    rank = base + inside
    over = jnp.max(jnp.max(base + num, axis=0, keepdims=True), axis=1, keepdims=True) > bound
    c64_s[:64, :] = jnp.where(sel, rank, -1.0)

    pair = jnp.full((TOK, ALL_EXP), -1.0, F32)
    for n in range(8):
        pair = jnp.where(log_s[...] == cand[n:n + 1, :], c64_s[pl.ds(me * 8 + n, 1), :], pair)
    r2_s[...] = pair.T
    la = log_s[...].T
    ex = jnp.exp(la - jnp.max(la, axis=0, keepdims=True))
    gt_s[...] = ex / jnp.sum(ex, axis=0, keepdims=True)

    await_bytes(seven, krecv)
    rv = rks[...]
    src = iota((64, ALL_EXP), 0) >> 3
    exp_chip = iota((64, ALL_EXP), 1) >> 6
    wide = jnp.max(jnp.max(jnp.where(sel & ((src >> 1) != exp_chip), rv, -1.0), axis=0, keepdims=True),
                   axis=1, keepdims=True) >= xb
    flag_out[0, 0] = jnp.max(jnp.where(over | wide, 1.0, 0.0)).astype(jnp.int32)
    rel = (src >> 1) ^ chip
    start = jnp.where(rel == 0, (src & 1) * TOK, 2 * TOK + (rel - 1) * xb).astype(F32)
    pos = start + rv + 1.0
    code = ((src >> 1) * 1024).astype(F32) + rank + 1.0
    pos_rows, code_rows = [], []
    for i in range(CAP):
        hit = sel & (slot == i)
        pos_rows.append(jnp.sum(jnp.where(hit, pos, 0.0), axis=0, keepdims=True))
        code_rows.append(jnp.sum(jnp.where(hit, code, 0.0), axis=0, keepdims=True))
    turn = ALL_EXP - me * EXP
    pos = pltpu.roll(jnp.concatenate(pos_rows, axis=0), turn, 1)
    code = pltpu.roll(jnp.concatenate(code_rows, axis=0), turn, 1)
    pio = iota((CAP, nx), 1).astype(F32) + 1.0
    for e in range(EXP):
        p_s[e * CAP:(e + 1) * CAP, :] = onehot(pos[:, e:e + 1] == pio)
        v_s[e * CAP:(e + 1) * CAP, :] = jnp.broadcast_to(code[:, e:e + 1], (CAP, 128))
    vt_s[...] = v_s[...].T[:8, :]
    rio = iota((bound, SLOTS), 0)
    for n, d in enumerate((xn, yn, dg, me)):
        want = (rio + ((d // 2) * 1024 + 1)).astype(F32)
        q_s[n * bound:(n + 1) * bound, :] = onehot(vt_s[0:1, :] == want)
    hacc[...] = jnp.zeros((SLOTS, FF), F32)

    def x_forward(c):
        await_bytes(xs.at[0], xrecv.at[c])
        x_fwd(c).start()

    def first_product(c, last):
        await_bytes(xs.at[0], xfrecv.at[c])
        lists = jnp.concatenate([xl[c, 0], xl[c, 1]], axis=1)
        near = own_s[c] if ahead_of else dot(p_s[:, :2 * TOK], xo[c])
        pick_s[...] = (near + dot(p_s[:, 2 * TOK:], lists)).astype(BF16)

        def group(g, _):
            i = c * groups + 2 * g
            w1_copy(i).wait()
            w1_copy(i + 1).wait()
            for j in range(2 * ge):
                rows = pl.ds(g * (2 * ge * CAP) + j * CAP, CAP)
                v = hacc[rows, :] + dot(pick_s[rows, :], w1buf[(i + j // ge) % ns1, j % ge])
                if last:
                    h_s[rows, :] = gelu(v).astype(BF16)
                else:
                    hacc[rows, :] = v

            for n in (i, i + 1):
                @pl.when(n + ns1 < items)
                def _():
                    w1_copy(n + ns1).start()

            return 0

        lax.fori_loop(0, groups // 2, group, 0)

    def chunk(c, _):
        x_forward(c + 1)
        first_product(c, False)
        return 0

    await_bytes(out_s, precv)
    x_forward(0)

    def pick_own(c, _):
        own_s[c] = dot(p_s[:, :2 * TOK], xo[c]).astype(BF16)
        return 0

    if ahead_of:
        lax.fori_loop(0, NC, pick_own, 0)
    lax.fori_loop(0, NC - 1, chunk, 0)
    first_product(NC - 1, True)

    RB = 64 if bound % 64 == 0 else 88

    def build_a(n, _):
        o = n // (bound // RB)
        r0 = (n % (bound // RB)) * RB
        rio2 = (iota((RB, TOK), 0) + r0).astype(F32)

        def one(e, acc):
            row = pl.ds(o * 2 * EXP + e, 1)
            return jnp.where(r2_s[row, :] == rio2, gt_s[row, :], acc)

        at_s[pl.ds(o * bound + r0, RB), :] = lax.fori_loop(0, 2 * EXP, one, jnp.zeros((RB, TOK), F32), unroll=8)
        return 0

    blocks = 4 * (bound // RB)
    per = blocks // NC + (blocks % NC > 0)

    def rblk(c, d):
        return recv.at[c, k, pl.ds((d // 2) * bound, bound), :]

    def q_copies(s):
        return (rcopy(zq.at[s, 1 - k], zin.at[s], qsend.at[s], qrecv.at[s], partner),
                rcopy(zq.at[s, k, pl.ds(3 * bound, bound), :], zown.at[s], qsend.at[s], qrecv.at[s], partner))

    def z_copy(c, n, dev):
        return rcopy(zs.at[c % nz, pl.ds(n * bound, bound), :], rblk(c, me), zsend.at[c % nz], zrecv.at[c], dev)

    def fwd_copy(c, d):
        return rcopy(rblk(c, d), rblk(c, d), zfsend, zfrecv.at[c], partner)

    def q_bytes(s):
        return zq.at[s, :, pl.ds(0, 5 * bound // 2), :]

    def merge(c):
        s = c % 2
        await_bytes(q_bytes(s), qrecv.at[s])
        if nz < NC:
            @pl.when(c >= nz)
            def _():
                await_bytes(zs.at[c % nz], zsend.at[c % nz])
        zs[c % nz] = zq[s, k, :3 * bound, :] + zin[s, :3 * bound, :]
        home = pl.ds(chip * bound, bound)
        recv[c, k, home, :] = zq[s, k, 3 * bound:, :] + zin[s, 3 * bound:, :]
        recv[c, 1 - k, home, :] = zq[s, 1 - k, 3 * bound:, :] + zown[s]
        for n, dev in ((2, dg), (0, xn), (1, yn)):
            z_copy(c, n, dev).start()

    def forward(c):
        await_bytes(zs.at[0], zrecv.at[c])
        for d in far:
            fwd_copy(c, d).start()

    def second_product(c, _):
        def group(g, _):
            i = c * groups + 2 * g
            w2_copy(i).wait()
            w2_copy(i + 1).wait()
            for j in range(2 * ge):
                rows = pl.ds(g * (2 * ge * CAP) + j * CAP, CAP)
                zc_s[rows, :] = dot(h_s[rows, :], w2buf[(i + j // ge) % ns2, j % ge]).astype(BF16)

            for n in (i, i + 1):
                @pl.when(n + ns2 < items)
                def _():
                    w2_copy(n + ns2).start()

            return 0

        lax.fori_loop(0, groups // 2, group, 0)
        @pl.when(c > 1)
        def _():
            merge(c - 1)
            await_bytes(q_bytes(c % 2), qsend.at[c % 2])

        zq_new = dot(q_s[...], zc_s[...]).astype(BF16)
        zq[c % 2, 0] = zq_new[:, :HW]
        zq[c % 2, 1] = zq_new[:, HW:]
        for copy in q_copies(c % 2):
            copy.start()

        @pl.when(c == 0)
        def _():
            merge(0)

        @pl.when(c > 1)
        def _():
            lax.fori_loop((c - 2) * per, (c - 1) * per, build_a, 0)

        @pl.when(c > 3)
        def _():
            forward(c - 4)

        return 0

    lax.fori_loop(0, NC, second_product, 0)
    merge(NC - 1)
    lax.fori_loop((NC - 2) * per, blocks, build_a, 0)
    def cut_a(j, _):
        a = at_s[pl.ds(j * 128, 128), :].T
        for n in range(3):
            part = a.astype(BF16)
            a_s[n, :, pl.ds(j * 128, 128)] = part
            a = a - part.astype(F32)
        return 0

    lax.fori_loop(0, rows_in // 128, cut_a, 0)

    def out_copy(c):
        return pltpu.make_async_copy(out_s.at[c], out.at[:, pl.ds(c * CW, CW)], osem)

    def combine(c):
        await_bytes(recv.at[c, 0, pl.ds(0, 3 * bound), :], zfrecv.at[c])
        z = jnp.concatenate([recv[c, 0], recv[c, 1]], axis=1)
        y = dot(a_s[2], z) + dot(a_s[1], z) + dot(a_s[0], z)
        out_s[c] = (xo[c, pl.ds(k * TOK, TOK), :].astype(F32) + y).astype(BF16)
        out_copy(c).start()

    def step(c, _):
        for at, chunk_in in ((1, 5), (6, 6), (6, 7)):
            @pl.when(c == at)
            def _():
                forward(chunk_in)

        combine(c)
        return 0

    await_bytes(seven, csend)
    await_bytes(seven, ksend)
    await_bytes(out_s, psend)
    for s in range(nz):
        await_bytes(xs.at[s], xsend.at[s])
    await_bytes(xl.at[:, 0], xfsend)
    forward(4)
    lax.fori_loop(0, NC, step, 0)
    log_swap.wait_send()
    for s in range(nq):
        await_bytes(xin.at[s], xqsend.at[s])
    for s in range(2):
        await_bytes(q_bytes(s), qsend.at[s])
    for s in range(nz):
        await_bytes(zs.at[s], zsend.at[s])
    await_bytes(recv.at[:, 0, pl.ds(0, 3 * bound), :], zfsend)
    await_bytes(out_s, osem)


def moe_call(xb, bound, ge, ns1, ns2, nz, lag, cid, tok, logit, w1, w2):
    nx = 2 * TOK + 3 * xb
    rows_in = -(-4 * bound // 128) * 128
    vm = pltpu.VMEM
    sem = pltpu.SemaphoreType.DMA
    sq = vm((ALL_EXP, TOK), F32)
    return pl.pallas_call(
        functools.partial(moe_kernel, xb, nx, bound, ge, ns1, ns2, nz, lag),
        out_shape=(jax.ShapeDtypeStruct((TOK, D), BF16), jax.ShapeDtypeStruct((1, 1), jnp.int32)),
        in_specs=[pl.BlockSpec(memory_space=pl.ANY)] * 4,
        out_specs=(pl.BlockSpec(memory_space=pl.ANY), pl.BlockSpec(memory_space=pltpu.SMEM)),
        scratch_shapes=[
            vm((NC, 2 * TOK, CW), BF16), vm((NC, 2, 3 * xb, HW), BF16), vm((2 * lag, 2, 3 * xb, HW), BF16),
            vm((2 * lag, 3 * xb, HW), BF16), vm((nz, 3 * xb, HW), BF16), sq,
            vm((ns1, ge, CW, FF), BF16), vm((ns2, ge, FF, CW), BF16),
            sq, vm((8, ALL_EXP), F32), vm((64, ALL_EXP), F32), vm((8, ALL_EXP), F32), vm((64, ALL_EXP), F32),
            vm((16, TOK), F32), vm((3 * xb, TOK), BF16), sq,
            vm((SLOTS, nx), BF16), vm((SLOTS, 128), F32), vm((8, SLOTS), F32), vm((4 * bound, SLOTS), BF16),
            vm((SLOTS, CW), BF16), vm((nz, SLOTS, CW), BF16), vm((SLOTS, FF), F32), vm((SLOTS, FF), BF16), vm((SLOTS, CW), BF16),
            vm((2, 2, 4 * bound, HW), BF16), vm((2, 4 * bound, HW), BF16), vm((2, bound, HW), BF16),
            vm((nz, 3 * bound, HW), BF16), vm((NC, 2, rows_in, HW), BF16),
            sq, sq, vm((rows_in, TOK), F32), vm((3, TOK, rows_in), BF16), vm((NC, TOK, CW), BF16),
            sem((ns1,)), sem((ns2,)), *[sem] * 7, sem((nz,)), *[sem] * 3, sem((NC,)), sem((NC,)),
            sem((nz,)), sem, sem((NC,)), sem((NC,)), sem((2,)), sem((2,)), sem((2 * lag,)), sem((2 * lag,)), sem, sem,
        ],
        compiler_params=pltpu.CompilerParams(collective_id=cid, has_side_effects=True, vmem_limit_bytes=67043328),
        name=f"moe_{bound}",
    )(tok, logit, w1, w2)


def solution(mesh):
    row_spec = P(("dp", "ep"), None)
    expert_spec = P("ep", None, None)

    def device_step(tok, logit, w1, w2):
        out, flag = moe_call(256, 352, 8, 7, 7, NC, 2, 0, tok, logit, w1, w2)
        return lax.switch(flag[0, 0], (lambda: out, lambda: moe_call(2 * TOK, 1024, 1, 2, 2, 1, 1, 1, tok, logit, w1, w2)[0]))

    return jax.shard_map(device_step, mesh=mesh, in_specs=(row_spec, row_spec, expert_spec, expert_spec),
                         out_specs=row_spec, check_vma=False)
```
